32 devices in a mesh: rep: 2 (over x), dp: 16 (over y, z, core).
Axes of the slice: x: 2, y: 2, z: 4, core: 2. Of those that a mesh axis runs over, the one named last changes fastest.
Arguments:
- x: bfloat16 [32, 2048, 512], P(('rep', 'dp')), parts along dimension 0
- dy: bfloat16 [32, 2048, 512], P(('rep', 'dp')), parts along dimension 0
- wq: bfloat16 [2, 512, 512], replicated
- wk: bfloat16 [2, 512, 512], replicated
- wv: bfloat16 [2, 512, 512], replicated
- wo: bfloat16 [2, 512, 512], replicated
- w_gate: bfloat16 [2, 512, 2048], replicated
- w_up: bfloat16 [2, 512, 2048], replicated
- w_down: bfloat16 [2, 2048, 512], replicated
- m_wq: float32 [2, 512, 512], P(None, 'dp')
- m_wk: float32 [2, 512, 512], P(None, 'dp')
- m_wv: float32 [2, 512, 512], P(None, 'dp')
- m_wo: float32 [2, 512, 512], P(None, 'dp')
- m_w_gate: float32 [2, 512, 2048], P(None, 'dp')
- m_w_up: float32 [2, 512, 2048], P(None, 'dp')
- m_w_down: float32 [2, 2048, 512], P(None, 'dp')
- v_wq: float32 [2, 512, 512], P(None, 'dp')
- v_wk: float32 [2, 512, 512], P(None, 'dp')
- v_wv: float32 [2, 512, 512], P(None, 'dp')
- v_wo: float32 [2, 512, 512], P(None, 'dp')
- v_w_gate: float32 [2, 512, 2048], P(None, 'dp')
- v_w_up: float32 [2, 512, 2048], P(None, 'dp')
- v_w_down: float32 [2, 2048, 512], P(None, 'dp')
Outputs:
- output 1: bfloat16 [4, 512, 512], P('rep'), parts along dimension 0
- output 2: bfloat16 [4, 512, 512], P('rep'), parts along dimension 0
- output 3: bfloat16 [4, 512, 512], P('rep'), parts along dimension 0
- output 4: bfloat16 [4, 512, 512], P('rep'), parts along dimension 0
- output 5: bfloat16 [4, 512, 2048], P('rep'), parts along dimension 0
- output 6: bfloat16 [4, 512, 2048], P('rep'), parts along dimension 0
- output 7: bfloat16 [4, 2048, 512], P('rep'), parts along dimension 0
- output 8: float32 [4, 512, 512], P('rep', 'dp'), parts along dimension 0
- output 9: float32 [4, 512, 512], P('rep', 'dp'), parts along dimension 0
- output 10: float32 [4, 512, 512], P('rep', 'dp'), parts along dimension 0
- output 11: float32 [4, 512, 512], P('rep', 'dp'), parts along dimension 0
- output 12: float32 [4, 512, 2048], P('rep', 'dp'), parts along dimension 0
- output 13: float32 [4, 512, 2048], P('rep', 'dp'), parts along dimension 0
- output 14: float32 [4, 2048, 512], P('rep', 'dp'), parts along dimension 0
- output 15: float32 [4, 512, 512], P('rep', 'dp'), parts along dimension 0
- output 16: float32 [4, 512, 512], P('rep', 'dp'), parts along dimension 0
- output 17: float32 [4, 512, 512], P('rep', 'dp'), parts along dimension 0
- output 18: float32 [4, 512, 512], P('rep', 'dp'), parts along dimension 0
- output 19: float32 [4, 512, 2048], P('rep', 'dp'), parts along dimension 0
- output 20: float32 [4, 512, 2048], P('rep', 'dp'), parts along dimension 0
- output 21: float32 [4, 2048, 512], P('rep', 'dp'), parts along dimension 0
There are 2 independent parts. The reference program is written for one: setup_inputs(seed, part) draws one part's arguments, and reference() takes and returns one part's arrays. A program takes and returns all parts, laid end to end along the dimension named above; an argument that names none is the same for every part.
All inputs are finite; a program needn't handle non-finite values.
Results may differ from the reference program's by a relative error of at most 0.024.
Values are sent between devices in bfloat16 or wider.
A program may use at most 2 GiB of HBM per device.

```python
import jax
import jax.numpy as jnp
from jax import lax

SEQUENCES = 16
TOKENS = 2048
D = 512
HEADS = 2
KV_HEADS = 2
HEAD = 256
FF = 2048
LAYERS = 2
THETA = 10000
NAMES = ("wq", "wk", "wv", "wo", "w_gate", "w_up", "w_down")
SHAPES = {
    "wq": (LAYERS, D, HEADS * HEAD),
    "wk": (LAYERS, D, KV_HEADS * HEAD),
    "wv": (LAYERS, D, KV_HEADS * HEAD),
    "wo": (LAYERS, HEADS * HEAD, D),
    "w_gate": (LAYERS, D, FF),
    "w_up": (LAYERS, D, FF),
    "w_down": (LAYERS, FF, D),
}


def bump(key, n, height):
    away = (jnp.arange(n, dtype=jnp.int32) - jax.random.randint(key, (), 0, n, jnp.int32)) % n
    return jnp.where(away < n // 8, height, 1.0)


def together(key, own, strength):
    shared = jax.random.normal(key, own.shape[1:], jnp.float32)
    return (own + strength * shared) * lax.rsqrt(1 + strength * strength)


def setup_inputs(seed: int = 0, part: int = 0) -> dict:
    kx, kdy, ka, kb, kz, kf, kh, kl, *keys = jax.random.split(jax.random.key(seed), 8 + 3 * len(NAMES))
    kx, kdy, ka, kb = (jax.random.fold_in(k, part) for k in (kx, kdy, ka, kb))
    kw, km, kv = (keys[i::3] for i in range(3))
    shape = (SEQUENCES, TOKENS, D)
    much_x, much_dy = jax.random.uniform(kz, (2,), jnp.float32, 0.0, 1.0)
    loud = 2.0 ** jax.random.uniform(jax.random.fold_in(kz, 1), (), jnp.float32, -1.0, 2.0)
    layers = 2.0 ** jax.random.uniform(kl, (LAYERS, 1, 1), jnp.float32, -1.0, 1.0)
    times = {"wq": 1.0, "wk": 1.0, "wv": 2.0, "wo": layers, "w_gate": 1.0, "w_up": bump(kh, FF, 4.0), "w_down": layers}
    x = together(ka, jax.random.normal(kx, shape, jnp.float32), much_x) * bump(kf, D, 4.0)
    dy = together(kb, jax.random.normal(kdy, shape, jnp.float32), much_dy)
    drawn = {"x": x.astype(jnp.bfloat16), "dy": (loud * dy * (SEQUENCES * TOKENS) ** -0.5).astype(jnp.bfloat16)}
    for key, name in zip(kw, NAMES, strict=True):
        drawn[name] = (jax.random.normal(key, SHAPES[name], jnp.float32) * SHAPES[name][1] ** -0.5 * times[name]).astype(jnp.bfloat16)
    for key, name in zip(km, NAMES, strict=True):
        drawn[f"m_{name}"] = 0.1 * jax.random.normal(key, SHAPES[name], jnp.float32)
    for key, name in zip(kv, NAMES, strict=True):
        drawn[f"v_{name}"] = loud * loud * jax.random.uniform(key, SHAPES[name], jnp.float32, 0.2, 0.6)
    return drawn


def matmul(a, w):
    return jnp.dot(a, w, preferred_element_type=jnp.float32).astype(jnp.bfloat16)


def normed(h):
    wide = h.astype(jnp.float32)
    scale = lax.rsqrt(jnp.mean(wide**2, -1, keepdims=True) + 1e-6)
    return (wide * scale).astype(jnp.bfloat16)


def turned(t, theta):
    half = t.shape[-1] // 2
    angle = jnp.arange(t.shape[0], dtype=jnp.float32)[:, None] * theta ** (-jnp.arange(half, dtype=jnp.float32) / half)
    cos, sin = jnp.cos(angle)[:, None], jnp.sin(angle)[:, None]
    a, b = t[..., :half].astype(jnp.float32), t[..., half:].astype(jnp.float32)
    return jnp.concatenate([a * cos - b * sin, b * cos + a * sin], -1).astype(jnp.bfloat16)


def seen_by(q, k, v):
    tokens, kv = q.shape[0], k.shape[1]
    q = q.reshape(tokens, kv, -1, q.shape[-1])
    scores = jnp.einsum("tgsd,ugd->gstu", q.astype(jnp.float32), k.astype(jnp.float32)) * q.shape[-1] ** -0.5
    place = jnp.arange(tokens)
    weights = jax.nn.softmax(jnp.where(place[:, None] >= place, scores, -jnp.inf), -1).astype(jnp.bfloat16)
    return jnp.einsum("gstu,ugd->tgsd", weights.astype(jnp.float32), v.astype(jnp.float32)).astype(jnp.bfloat16).reshape(tokens, -1)


def layer(h, w):
    a = normed(h)
    q, k = (turned(matmul(a, w[name]).reshape(h.shape[0], -1, HEAD), THETA) for name in ("wq", "wk"))
    h = h + matmul(seen_by(q, k, matmul(a, w["wv"]).reshape(h.shape[0], -1, HEAD)), w["wo"])
    b = normed(h)
    gate = jnp.dot(b, w["w_gate"], preferred_element_type=jnp.float32)
    up = jnp.dot(b, w["w_up"], preferred_element_type=jnp.float32)
    return h + matmul((jax.nn.silu(gate) * up).astype(jnp.bfloat16), w["w_down"])


def adamw(w, m, v, g):
    m = 0.9 * m + 0.1 * g
    v = 0.95 * v + 0.05 * g * g
    step = m * lax.rsqrt(v + 1e-8) + 0.1 * w
    return (w - 0.02 * step).astype(jnp.bfloat16), m, v


def stack(weights, h):
    return lax.scan(lambda h, w: (layer(h, w), None), h, weights)[0]


def reference(x, dy, wq, wk, wv, wo, w_gate, w_up, w_down, m_wq, m_wk, m_wv, m_wo, m_w_gate, m_w_up, m_w_down, v_wq, v_wk, v_wv, v_wo, v_w_gate, v_w_up, v_w_down):
    weights = dict(zip(NAMES, (wq, wk, wv, wo, w_gate, w_up, w_down), strict=True))

    def take(so_far, sequence):
        h, by_y = sequence
        _, back = jax.vjp(stack, weights, h)
        by_weights, by_h = back(by_y)
        return jax.tree.map(lambda total, term: total + term.astype(jnp.float32), so_far, by_weights), by_h

    none_yet = {name: jnp.zeros(w.shape, jnp.float32) for name, w in weights.items()}
    by_weights, by_x = lax.scan(take, none_yet, (x, dy))
    gradients = [by_weights[name].astype(jnp.bfloat16).astype(jnp.float32) for name in NAMES]
    first = (m_wq, m_wk, m_wv, m_wo, m_w_gate, m_w_up, m_w_down)
    second = (v_wq, v_wk, v_wv, v_wo, v_w_gate, v_w_up, v_w_down)
    new = [adamw(weights[name].astype(jnp.float32), m, v, g) for name, m, v, g in zip(NAMES, first, second, gradients, strict=True)]
    return tuple(one[which] for which in range(3) for one in new)
```

```python
import functools

import jax
import jax.numpy as jnp
import numpy as np
from jax import lax
from jax.experimental import pallas as pl
from jax.experimental.pallas import tpu as pltpu
from jax.sharding import PartitionSpec as P

LOG2E = 1.4426950408889634
BF, F32 = jnp.bfloat16, jnp.float32
D, HEAD, HEADS, FF, S = 512, 256, 2, 2048, 2048
HALF = HEAD // 2
THETA = 10000
STRIP = 512
N_STRIP = S // STRIP
E = HEAD**-0.5 * LOG2E
HIDDEN = -2e30


def _dot(a, b, ca=1, cb=0):
    return lax.dot_general(a, b, (((ca,), (cb,)), ((), ())), preferred_element_type=F32)


def _scale_of(wide):
    return lax.rsqrt(jnp.mean(wide * wide, -1, keepdims=True) + 1e-6)


def _normed(h):
    wide = h.astype(F32)
    return (wide * _scale_of(wide)).astype(BF)


def _norm_back(h, ct):
    wide = h.astype(F32)
    scale = _scale_of(wide)
    return ct * scale - wide * (scale * scale * scale * jnp.mean(ct * wide, -1, keepdims=True))


def _params(vmem, grid=1):
    return pltpu.CompilerParams(dimension_semantics=("arbitrary",) * grid, vmem_limit_bytes=int(vmem * 2**20))


def _cost(flops, nbytes, trans=0):
    return pl.CostEstimate(flops=int(flops), bytes_accessed=int(nbytes), transcendentals=int(trans))


def _rows(tb, width=D):
    return pl.BlockSpec((tb, width), lambda t: (t, 0))


def _weight(layer, *shape):
    return pl.BlockSpec((None, *shape), lambda *_: (layer, 0, 0))


def _whole(*shape):
    return pl.BlockSpec(shape, lambda *_: (0,) * len(shape))


def _turn(t, cos, sin):
    out = []
    for i in range(HEADS):
        a = t[:, i * HEAD : i * HEAD + HALF].astype(F32)
        b = t[:, i * HEAD + HALF : (i + 1) * HEAD].astype(F32)
        out += [a * cos - b * sin, b * cos + a * sin]
    return jnp.concatenate(out, -1).astype(BF)


def _turn_back(t, cos, sin):
    out = []
    for i in range(HEADS):
        a = t[:, i * HEAD : i * HEAD + HALF].astype(F32)
        b = t[:, i * HEAD + HALF : (i + 1) * HEAD].astype(F32)
        out += [a * cos + b * sin, b * cos - a * sin]
    return jnp.concatenate(out, -1).astype(BF)


def _qkv_kernel(h_ref, cos_ref, sin_ref, wq_ref, wk_ref, wv_ref, q_ref, k_ref, v_ref):
    a = _normed(h_ref[...])
    cos, sin = cos_ref[...], sin_ref[...]
    q_ref[...] = _turn(_dot(a, wq_ref[...]).astype(BF), cos, sin)
    k_ref[...] = _turn(_dot(a, wk_ref[...]).astype(BF), cos, sin)
    v_ref[...] = _dot(a, wv_ref[...]).astype(BF)


def qkv(layer, h, cos, sin, wq, wk, wv, tb=512):
    one = jax.ShapeDtypeStruct((S, D), BF)
    w = _weight(layer, D, D)
    return pl.pallas_call(
        _qkv_kernel, grid=(S // tb,), name="qkv",
        in_specs=[_rows(tb), _rows(tb, HALF), _rows(tb, HALF), w, w, w],
        out_specs=[_rows(tb)] * 3, out_shape=[one] * 3,
        compiler_params=_params(32), cost_estimate=_cost(3 * 2 * S * D * D, 4 * S * D * 2 + 2 * S * HALF * 4),
    )(h, cos, sin, wq, wk, wv)


def _diag():
    shape = (STRIP, STRIP)
    return lax.broadcasted_iota(jnp.int32, shape, 1) >= lax.broadcasted_iota(jnp.int32, shape, 0)


def _attend_kernel(q_ref, k_ref, v_ref, o_ref, lse_ref, vt_s, sc_s, p_s):
    ok = _diag()
    for i in range(HEADS):
        col = slice(i * HEAD, (i + 1) * HEAD)
        vt_s[i, :HEAD, :] = v_ref[:, col].T
        vt_s[i, HEAD:, :] = jnp.ones((16, S), BF)
    for s in range(N_STRIP):
        for i in range(HEADS):
            col = slice(i * HEAD, (i + 1) * HEAD)
            here = slice(s * STRIP, (s + 1) * STRIP)
            n = (s + 1) * STRIP
            q = q_ref[here, col]
            top = None
            for j in range(s + 1):
                sc = _dot(k_ref[j * STRIP : (j + 1) * STRIP, col], q, 1, 1)
                if j == s:
                    sc = jnp.where(ok, sc, HIDDEN)
                sc_s[i, j * STRIP : (j + 1) * STRIP, :] = sc
                m = sc.max(axis=0, keepdims=True)
                top = m if top is None else jnp.maximum(top, m)
            for j in range(s + 1):
                at = slice(j * STRIP, (j + 1) * STRIP)
                p_s[i, at, :] = jnp.exp2((sc_s[i, at, :] - top) * E).astype(BF)
            mix = _dot(vt_s[i, :, :n], p_s[i, :n, :])
            total = mix[HEAD : HEAD + 1, :]
            o_ref[here, col] = (mix[:HEAD, :] * (1 / total)).T.astype(BF)
            lse_ref[i : i + 1, here] = top * (HEAD**-0.5) + jnp.log(total)


def attend(q, k, v):
    return pl.pallas_call(
        _attend_kernel, grid=(1,), name="attend",
        in_specs=[_whole(S, D)] * 3, out_specs=[_whole(S, D), _whole(8, S)],
        out_shape=[jax.ShapeDtypeStruct((S, D), BF), jax.ShapeDtypeStruct((8, S), F32)],
        scratch_shapes=[pltpu.VMEM((HEADS, HEAD + 16, S), BF), pltpu.VMEM((HEADS, S, STRIP), F32), pltpu.VMEM((HEADS, S, STRIP), BF)],
        compiler_params=_params(48), cost_estimate=_cost(2 * HEADS * S * S * HEAD * 1.25, 8 * S * D, HEADS * S * S * 0.6),
    )(q, k, v)


def _attend_back_kernel(q_ref, k_ref, v_ref, o_ref, do_ref, lse_ref, dq_ref, dk_ref, dv_ref, dq_s, p_s, ds_s):
    ok = _diag()
    for i in range(HEADS):
        col = slice(i * HEAD, (i + 1) * HEAD)
        lse = lse_ref[i : i + 1, :] * LOG2E
        deltas = []
        for s in range(N_STRIP):
            here = slice(s * STRIP, (s + 1) * STRIP)
            both = do_ref[here, col].astype(F32) * o_ref[here, col].astype(F32)
            delta = both.sum(-1, keepdims=True)
            deltas.append(jnp.broadcast_to(delta, (STRIP, 128)).T[0:1, :])
        for j in range(N_STRIP):
            at = slice(j * STRIP, (j + 1) * STRIP)
            k, v = k_ref[at, col], v_ref[at, col]
            kt = k.T
            for s in range(j, N_STRIP):
                here = slice(s * STRIP, (s + 1) * STRIP)
                p = jnp.exp2(_dot(k, q_ref[here, col], 1, 1) * E - lse[:, here])
                if s == j:
                    p = jnp.where(ok, p, 0.0)
                dp = _dot(v, do_ref[here, col], 1, 1)
                ds = (p * (dp - deltas[s])).astype(BF)
                p_s[i, :, here] = p.astype(BF)
                ds_s[i, :, here] = ds
                part = _dot(kt, ds)
                if j == 0:
                    dq_s[i, :, here] = part
                else:
                    dq_s[i, :, here] += part
            rest = slice(j * STRIP, S)
            dv_ref[at, col] = _dot(p_s[i, :, rest], do_ref[rest, col]).astype(BF)
            dk_ref[at, col] = (_dot(ds_s[i, :, rest], q_ref[rest, col]) * (HEAD**-0.5)).astype(BF)
        dq_ref[:, col] = (dq_s[i] * (HEAD**-0.5)).T.astype(BF)


def attend_back(q, k, v, o, do, lse):
    one = jax.ShapeDtypeStruct((S, D), BF)
    return pl.pallas_call(
        _attend_back_kernel, grid=(1,), name="attend_back",
        in_specs=[_whole(S, D)] * 5 + [_whole(8, S)], out_specs=[_whole(S, D)] * 3, out_shape=[one] * 3,
        scratch_shapes=[pltpu.VMEM((HEADS, HEAD, S), F32), pltpu.VMEM((HEADS, STRIP, S), BF), pltpu.VMEM((HEADS, STRIP, S), BF)],
        compiler_params=_params(56), cost_estimate=_cost(5 * HEADS * S * S * HEAD * 1.25, 16 * S * D, HEADS * S * S * 0.6),
    )(q, k, v, o, do, lse)


def _project_kernel(h_ref, o_ref, wo_ref, h1_ref):
    h1_ref[...] = (h_ref[...].astype(F32) + _dot(o_ref[...], wo_ref[...]).astype(BF).astype(F32)).astype(BF)


def project(layer, h, o, wo, tb=512):
    return pl.pallas_call(
        _project_kernel, grid=(S // tb,), name="project",
        in_specs=[_rows(tb), _rows(tb), _weight(layer, D, D)], out_specs=_rows(tb), out_shape=jax.ShapeDtypeStruct((S, D), BF),
        compiler_params=_params(32), cost_estimate=_cost(2 * S * D * D, 6 * S * D),
    )(h, o, wo)


def _ffn_kernel(h_ref, o_ref, wo_ref, wg_ref, wu_ref, wd_ref, h1_ref, h2_ref, act_s, *, fc):
    h1 = (h_ref[...].astype(F32) + _dot(o_ref[...], wo_ref[...]).astype(BF).astype(F32)).astype(BF)
    h1_ref[...] = h1
    b = _normed(h1)
    for c in range(FF // fc):
        at = slice(c * fc, (c + 1) * fc)
        gate, up = _dot(b, wg_ref[:, at]), _dot(b, wu_ref[:, at])
        act_s[:, at] = (gate * jax.nn.sigmoid(gate) * up).astype(BF)
    h2_ref[...] = (h1.astype(F32) + _dot(act_s[...], wd_ref[...]).astype(BF).astype(F32)).astype(BF)


def ffn(layer, h, o, wo, wg, wu, wd, tb=512, fc=512):
    one = jax.ShapeDtypeStruct((S, D), BF)
    return pl.pallas_call(
        functools.partial(_ffn_kernel, fc=fc), grid=(S // tb,), name="ffn",
        in_specs=[_rows(tb), _rows(tb), _weight(layer, D, D), _weight(layer, D, FF), _weight(layer, D, FF), _weight(layer, FF, D)],
        out_specs=[_rows(tb)] * 2, out_shape=[one] * 2, scratch_shapes=[pltpu.VMEM((tb, FF), BF)],
        compiler_params=_params(48), cost_estimate=_cost(2 * S * D * (D + 3 * FF), 8 * S * D + 6 * D * FF, S * FF),
    )(h, o, wo, wg, wu, wd)


def _ffn_back_kernel(dy_ref, h1_ref, wo_ref, wg_ref, wu_ref, wd_ref, dh1_ref, do_ref, g_ref, dg_s, du_s, ag_s, au_s, ad_s, *, fc, order):
    t = pl.program_id(0)

    @pl.when(t == 0)
    def _():
        for ref in (ag_s, au_s, ad_s):
            ref[...] = jnp.zeros_like(ref)

    dy, h1 = dy_ref[...], h1_ref[...]
    b = _normed(h1)
    bt, dyt = b.T, dy.T
    for c in range(FF // fc):
        at = slice(c * fc, (c + 1) * fc)
        gate, up = _dot(b, wg_ref[:, at]), _dot(b, wu_ref[:, at])
        dact = _dot(dy, wd_ref[at, :], 1, 1).astype(BF).astype(F32)
        sig = jax.nn.sigmoid(gate)
        silu = gate * sig
        act = (silu * up).astype(BF)
        du = (dact * silu).astype(BF)
        dg = (dact * up * (sig + silu * (1 - sig))).astype(BF)
        dg_s[:, at] = dg
        du_s[:, at] = du
        ag_s[:, at] += _dot(bt, dg)
        au_s[:, at] += _dot(bt, du)
        ad_s[:, at] += _dot(dyt, act)
    db = (_dot(dg_s[...], wg_ref[...], 1, 1) + _dot(du_s[...], wu_ref[...], 1, 1)).astype(BF).astype(F32)
    dh1 = (dy.astype(F32) + _norm_back(h1, db).astype(BF).astype(F32)).astype(BF)
    dh1_ref[...] = dh1
    do_ref[...] = _dot(dh1, wo_ref[...], 1, 1).astype(BF)

    @pl.when(t == pl.num_programs(0) - 1)
    def _():
        n = len(order)
        r, f = D // n, FF // n
        for i, to in enumerate(order):
            for c in range(FF // D):
                at = slice(c * D, (c + 1) * D)
                g_ref[to, c * r : (c + 1) * r, :] = ag_s[i * r : (i + 1) * r, at].astype(BF)
                g_ref[to, f + c * r : f + (c + 1) * r, :] = au_s[i * r : (i + 1) * r, at].astype(BF)
            g_ref[to, 2 * f : 3 * f, :] = ad_s[:, i * f : (i + 1) * f].T.astype(BF)


def ffn_back(layer, order, dy, h1, wo, wg, wu, wd, tb=512, fc=512):
    one, n = jax.ShapeDtypeStruct((S, D), BF), len(order)
    return pl.pallas_call(
        functools.partial(_ffn_back_kernel, fc=fc, order=order), grid=(S // tb,), name="ffn_back",
        in_specs=[_rows(tb), _rows(tb), _weight(layer, D, D), _weight(layer, D, FF), _weight(layer, D, FF), _weight(layer, FF, D)],
        out_specs=[_rows(tb), _rows(tb), _whole(n, 3 * FF // n, D)],
        out_shape=[one, one, jax.ShapeDtypeStruct((n, 3 * FF // n, D), BF)],
        scratch_shapes=[pltpu.VMEM((tb, FF), BF)] * 2 + [pltpu.VMEM((D, FF), F32)] * 3,
        compiler_params=_params(63.9), cost_estimate=_cost(2 * S * D * (D + 8 * FF), 8 * S * D + 12 * D * FF, S * FF),
    )(dy, h1, wo, wg, wu, wd)


def _qkv_back_kernel(dq_ref, dk_ref, dv_ref, cos_ref, sin_ref, h_ref, dh1_ref, o_ref, wq_ref, wk_ref, wv_ref, dh_ref, g_ref, acc_s, *, order):
    t = pl.program_id(0)

    @pl.when(t == 0)
    def _():
        acc_s[...] = jnp.zeros_like(acc_s)

    cos, sin = cos_ref[...], sin_ref[...]
    dq, dk, dv = _turn_back(dq_ref[...], cos, sin), _turn_back(dk_ref[...], cos, sin), dv_ref[...]
    h, dh1 = h_ref[...], dh1_ref[...]
    at = _normed(h).T
    acc_s[0] += _dot(at, dq)
    acc_s[1] += _dot(at, dk)
    acc_s[2] += _dot(at, dv)
    acc_s[3] += _dot(o_ref[...].T, dh1)
    if dh_ref is not None:
        da = (_dot(dq, wq_ref[...], 1, 1) + _dot(dk, wk_ref[...], 1, 1) + _dot(dv, wv_ref[...], 1, 1)).astype(BF).astype(F32)
        dh_ref[...] = (dh1.astype(F32) + _norm_back(h, da).astype(BF).astype(F32)).astype(BF)

    @pl.when(t == pl.num_programs(0) - 1)
    def _():
        r = D // len(order)
        for i, to in enumerate(order):
            for c in range(4):
                g_ref[to, c * r : (c + 1) * r, :] = acc_s[c, i * r : (i + 1) * r, :].astype(BF)


def qkv_back(layer, order, dq, dk, dv, cos, sin, h, dh1, o, wq, wk, wv, tb=512):
    w, first, n = _weight(layer, D, D), layer == 0, len(order)
    packed = jax.ShapeDtypeStruct((n, 4 * D // n, D), BF)
    if first:
        def body(*refs, order):
            _qkv_back_kernel(*refs[:8], None, None, None, None, *refs[8:], order=order)
    else:
        body = _qkv_back_kernel
    given = [dq, dk, dv, cos, sin, h, dh1, o] + ([] if first else [wq, wk, wv])
    got = pl.pallas_call(
        functools.partial(body, order=order), grid=(S // tb,), name="qkv_back",
        in_specs=[_rows(tb)] * 3 + [_rows(tb, HALF)] * 2 + [_rows(tb)] * 3 + ([] if first else [w] * 3),
        out_specs=([] if first else [_rows(tb)]) + [_whole(n, 4 * D // n, D)],
        out_shape=([] if first else [jax.ShapeDtypeStruct((S, D), BF)]) + [packed],
        scratch_shapes=[pltpu.VMEM((4, D, D), F32)],
        compiler_params=_params(48), cost_estimate=_cost(2 * S * D * D * (4 if first else 7), 14 * S * D),
    )(*given)
    return (None, got[0]) if first else got


def tables():
    rate = THETA ** (-np.arange(HALF) / HALF)
    low, high = np.arange(128)[:, None] * rate, np.arange(S // 128)[:, None] * 128 * rate
    cl, sl, ch, sh = (jnp.asarray(f(x), F32) for x in (low, high) for f in (np.cos, np.sin))
    cl, sl, ch, sh = cl[None], sl[None], ch[:, None], sh[:, None]
    return (ch * cl - sh * sl).reshape(S, HALF), (sh * cl + ch * sl).reshape(S, HALF)


def adamw(w, m, v, g):
    m = 0.9 * m + 0.1 * g
    v = 0.95 * v + 0.05 * g * g
    step = m * lax.rsqrt(v + 1e-8) + 0.1 * w
    return (w - 0.02 * step).astype(BF), m, v


def solution(mesh):
    n = mesh.shape["dp"]
    order = tuple(range(n))

    def step(x, dy, wq, wk, wv, wo, wg, wu, wd, *moments):
        cos, sin = tables()
        h0 = x[0]
        q0, k0, v0 = qkv(0, h0, cos, sin, wq, wk, wv)
        o0, l0 = attend(q0, k0, v0)
        m0, h1 = ffn(0, h0, o0, wo, wg, wu, wd)
        q1, k1, v1 = qkv(1, h1, cos, sin, wq, wk, wv)
        o1, l1 = attend(q1, k1, v1)
        m1 = project(1, h1, o1, wo)
        dm1, do1, gf1 = ffn_back(1, order, dy[0], m1, wo, wg, wu, wd)
        dq1, dk1, dv1 = attend_back(q1, k1, v1, o1, do1, l1)
        dh1, ga1 = qkv_back(1, order, dq1, dk1, dv1, cos, sin, h1, dm1, o1, wq, wk, wv)
        dm0, do0, gf0 = ffn_back(0, order, dh1, m0, wo, wg, wu, wd)
        dq0, dk0, dv0 = attend_back(q0, k0, v0, o0, do0, l0)
        _, ga0 = qkv_back(0, order, dq0, dk0, dv0, cos, sin, h0, dm0, o0, wq, wk, wv)
        rs = lambda g: lax.psum_scatter(g, "dp", scatter_dimension=0, tiled=False).astype(F32)
        r, f = D // n, FF // n
        gf1, mid, ga0 = rs(gf1), rs(jnp.concatenate([ga1, gf0], 1)), rs(ga0)
        ga, gf = [ga0, mid[: 4 * r]], [mid[4 * r :], gf1]
        wide = lambda g: jnp.concatenate([g[c * r : (c + 1) * r] for c in range(FF // D)], 1)
        grads = [jnp.stack([g[c * r : (c + 1) * r] for g in ga]) for c in range(4)]
        grads += [jnp.stack([wide(g[c * f : (c + 1) * f]) for g in gf]) for c in range(2)]
        grads += [jnp.stack([g[2 * f :] for g in gf])]
        me = lax.axis_index("dp")
        weights, m, v = (wq, wk, wv, wo, wg, wu, wd), moments[:7], moments[7:]
        own = [lax.dynamic_slice_in_dim(w, me * one.shape[1], one.shape[1], 1).astype(F32) for w, one in zip(weights, m, strict=True)]
        new = [adamw(w, m, v, g) for w, m, v, g in zip(own, m, v, grads, strict=True)]
        flat = [one[0] for one in new]
        flat = [w if w.shape[2] == D else jnp.concatenate([w[:, :, c * D : (c + 1) * D] for c in range(FF // D)], 1) for w in flat]
        whole = lax.all_gather(jnp.concatenate(flat, 1), "dp", axis=0, tiled=False)
        out, at = [], 0
        for w, one in zip(weights, flat, strict=True):
            part = whole[:, :, at : at + one.shape[1]]
            at += one.shape[1]
            if w.shape[2] != D:
                part = part.reshape(n, 2, FF // D, r, D).transpose(1, 0, 3, 2, 4)
            else:
                part = part.transpose(1, 0, 2, 3)
            out.append(part.reshape(w.shape))
        return (*out, *(one[1] for one in new), *(one[2] for one in new))

    states, all_of, cut = P(("rep", "dp"), None, None), P(None, None, None), P(None, "dp", None)
    return jax.shard_map(
        step, mesh=mesh, in_specs=(states, states) + (all_of,) * 7 + (cut,) * 14,
        out_specs=(P("rep", None, None),) * 7 + (P("rep", "dp", None),) * 14, check_vma=False,
    )
```

```python
import functools

import jax
import jax.numpy as jnp
import numpy as np
from jax import lax
from jax.experimental import pallas as pl
from jax.experimental.pallas import tpu as pltpu
from jax.sharding import PartitionSpec as P

LOG2E = 1.4426950408889634
BF, F32 = jnp.bfloat16, jnp.float32
D, HEAD, HEADS, FF, S = 512, 256, 2, 2048, 2048
HALF = HEAD // 2
THETA = 10000
STRIP = 512
N_STRIP = S // STRIP
E = HEAD**-0.5 * LOG2E
HIDDEN = -2e30


def _dot(a, b, ca=1, cb=0):
    return lax.dot_general(a, b, (((ca,), (cb,)), ((), ())), preferred_element_type=F32)


def _scale_of(wide):
    return lax.rsqrt(jnp.mean(wide * wide, -1, keepdims=True) + 1e-6)


def _normed(h):
    wide = h.astype(F32)
    return (wide * _scale_of(wide)).astype(BF)


def _norm_back(h, ct):
    wide = h.astype(F32)
    scale = _scale_of(wide)
    return ct * scale - wide * (scale * scale * scale * jnp.mean(ct * wide, -1, keepdims=True))


def _params(vmem, grid=1):
    return pltpu.CompilerParams(dimension_semantics=("arbitrary",) * grid, vmem_limit_bytes=int(vmem * 2**20))


def _cost(flops, nbytes, trans=0):
    return pl.CostEstimate(flops=int(flops), bytes_accessed=int(nbytes), transcendentals=int(trans))


def _rows(tb, width=D):
    return pl.BlockSpec((tb, width), lambda t: (t, 0))


def _weight(layer, *shape):
    return pl.BlockSpec((None, *shape), lambda *_: (layer, 0, 0))


def _whole(*shape):
    return pl.BlockSpec(shape, lambda *_: (0,) * len(shape))


def _turn(t, cos, sin):
    out = []
    for i in range(HEADS):
        a = t[:, i * HEAD : i * HEAD + HALF].astype(F32)
        b = t[:, i * HEAD + HALF : (i + 1) * HEAD].astype(F32)
        out += [a * cos - b * sin, b * cos + a * sin]
    return jnp.concatenate(out, -1).astype(BF)


def _turn_back(t, cos, sin):
    out = []
    for i in range(HEADS):
        a = t[:, i * HEAD : i * HEAD + HALF].astype(F32)
        b = t[:, i * HEAD + HALF : (i + 1) * HEAD].astype(F32)
        out += [a * cos + b * sin, b * cos - a * sin]
    return jnp.concatenate(out, -1).astype(BF)


def _qkv_kernel(h_ref, cos_ref, sin_ref, wq_ref, wk_ref, wv_ref, q_ref, k_ref, v_ref):
    a = _normed(h_ref[...])
    cos, sin = cos_ref[...], sin_ref[...]
    q_ref[...] = _turn(_dot(a, wq_ref[...]).astype(BF), cos, sin)
    k_ref[...] = _turn(_dot(a, wk_ref[...]).astype(BF), cos, sin)
    v_ref[...] = _dot(a, wv_ref[...]).astype(BF)


def qkv(layer, h, cos, sin, wq, wk, wv, tb=512):
    one = jax.ShapeDtypeStruct((S, D), BF)
    w = _weight(layer, D, D)
    return pl.pallas_call(
        _qkv_kernel, grid=(S // tb,), name="qkv",
        in_specs=[_rows(tb), _rows(tb, HALF), _rows(tb, HALF), w, w, w],
        out_specs=[_rows(tb)] * 3, out_shape=[one] * 3,
        compiler_params=_params(32), cost_estimate=_cost(3 * 2 * S * D * D, 4 * S * D * 2 + 2 * S * HALF * 4),
    )(h, cos, sin, wq, wk, wv)


def _diag():
    shape = (STRIP, STRIP)
    return lax.broadcasted_iota(jnp.int32, shape, 1) >= lax.broadcasted_iota(jnp.int32, shape, 0)


def _attend_kernel(q_ref, k_ref, v_ref, o_ref, lse_ref, vt_s, sc_s, p_s):
    ok = _diag()
    for i in range(HEADS):
        col = slice(i * HEAD, (i + 1) * HEAD)
        vt_s[i, :HEAD, :] = v_ref[:, col].T
        vt_s[i, HEAD:, :] = jnp.ones((16, S), BF)
    for s in range(N_STRIP):
        for i in range(HEADS):
            col = slice(i * HEAD, (i + 1) * HEAD)
            here = slice(s * STRIP, (s + 1) * STRIP)
            n = (s + 1) * STRIP
            q = q_ref[here, col]
            top = None
            for j in range(s + 1):
                sc = _dot(k_ref[j * STRIP : (j + 1) * STRIP, col], q, 1, 1)
                if j == s:
                    sc = jnp.where(ok, sc, HIDDEN)
                sc_s[i, j * STRIP : (j + 1) * STRIP, :] = sc
                m = sc.max(axis=0, keepdims=True)
                top = m if top is None else jnp.maximum(top, m)
            for j in range(s + 1):
                at = slice(j * STRIP, (j + 1) * STRIP)
                p_s[i, at, :] = jnp.exp2((sc_s[i, at, :] - top) * E).astype(BF)
            mix = _dot(vt_s[i, :, :n], p_s[i, :n, :])
            total = mix[HEAD : HEAD + 1, :]
            o_ref[here, col] = (mix[:HEAD, :] * (1 / total)).T.astype(BF)
            lse_ref[i : i + 1, here] = top * (HEAD**-0.5) + jnp.log(total)


def attend(q, k, v):
    return pl.pallas_call(
        _attend_kernel, grid=(1,), name="attend",
        in_specs=[_whole(S, D)] * 3, out_specs=[_whole(S, D), _whole(8, S)],
        out_shape=[jax.ShapeDtypeStruct((S, D), BF), jax.ShapeDtypeStruct((8, S), F32)],
        scratch_shapes=[pltpu.VMEM((HEADS, HEAD + 16, S), BF), pltpu.VMEM((HEADS, S, STRIP), F32), pltpu.VMEM((HEADS, S, STRIP), BF)],
        compiler_params=_params(48), cost_estimate=_cost(2 * HEADS * S * S * HEAD * 1.25, 8 * S * D, HEADS * S * S * 0.6),
    )(q, k, v)


def _attend_back_kernel(q_ref, k_ref, v_ref, o_ref, do_ref, lse_ref, dq_ref, dk_ref, dv_ref, dq_s, p_s, ds_s):
    ok = _diag()
    for i in range(HEADS):
        col = slice(i * HEAD, (i + 1) * HEAD)
        lse = lse_ref[i : i + 1, :] * LOG2E
        deltas = []
        for s in range(N_STRIP):
            here = slice(s * STRIP, (s + 1) * STRIP)
            both = do_ref[here, col].astype(F32) * o_ref[here, col].astype(F32)
            delta = both.sum(-1, keepdims=True)
            deltas.append(jnp.broadcast_to(delta, (STRIP, 128)).T[0:1, :])
        for j in range(N_STRIP):
            at = slice(j * STRIP, (j + 1) * STRIP)
            k, v = k_ref[at, col], v_ref[at, col]
            kt = k.T
            for s in range(j, N_STRIP):
                here = slice(s * STRIP, (s + 1) * STRIP)
                p = jnp.exp2(_dot(k, q_ref[here, col], 1, 1) * E - lse[:, here])
                if s == j:
                    p = jnp.where(ok, p, 0.0)
                dp = _dot(v, do_ref[here, col], 1, 1)
                ds = (p * (dp - deltas[s])).astype(BF)
                p_s[i, :, here] = p.astype(BF)
                ds_s[i, :, here] = ds
                part = _dot(kt, ds)
                if j == 0:
                    dq_s[i, :, here] = part
                else:
                    dq_s[i, :, here] += part
            rest = slice(j * STRIP, S)
            dv_ref[at, col] = _dot(p_s[i, :, rest], do_ref[rest, col]).astype(BF)
            dk_ref[at, col] = (_dot(ds_s[i, :, rest], q_ref[rest, col]) * (HEAD**-0.5)).astype(BF)
        dq_ref[:, col] = (dq_s[i] * (HEAD**-0.5)).T.astype(BF)


def attend_back(q, k, v, o, do, lse):
    one = jax.ShapeDtypeStruct((S, D), BF)
    return pl.pallas_call(
        _attend_back_kernel, grid=(1,), name="attend_back",
        in_specs=[_whole(S, D)] * 5 + [_whole(8, S)], out_specs=[_whole(S, D)] * 3, out_shape=[one] * 3,
        scratch_shapes=[pltpu.VMEM((HEADS, HEAD, S), F32), pltpu.VMEM((HEADS, STRIP, S), BF), pltpu.VMEM((HEADS, STRIP, S), BF)],
        compiler_params=_params(56), cost_estimate=_cost(5 * HEADS * S * S * HEAD * 1.25, 16 * S * D, HEADS * S * S * 0.6),
    )(q, k, v, o, do, lse)


def _project_kernel(h_ref, o_ref, wo_ref, h1_ref):
    h1_ref[...] = (h_ref[...].astype(F32) + _dot(o_ref[...], wo_ref[...]).astype(BF).astype(F32)).astype(BF)


def project(layer, h, o, wo, tb=512):
    return pl.pallas_call(
        _project_kernel, grid=(S // tb,), name="project",
        in_specs=[_rows(tb), _rows(tb), _weight(layer, D, D)], out_specs=_rows(tb), out_shape=jax.ShapeDtypeStruct((S, D), BF),
        compiler_params=_params(32), cost_estimate=_cost(2 * S * D * D, 6 * S * D),
    )(h, o, wo)


def _ffn_kernel(h_ref, o_ref, wo_ref, wg_ref, wu_ref, wd_ref, h1_ref, h2_ref, act_s, *, fc):
    h1 = (h_ref[...].astype(F32) + _dot(o_ref[...], wo_ref[...]).astype(BF).astype(F32)).astype(BF)
    h1_ref[...] = h1
    b = _normed(h1)
    for c in range(FF // fc):
        at = slice(c * fc, (c + 1) * fc)
        gate, up = _dot(b, wg_ref[:, at]), _dot(b, wu_ref[:, at])
        act_s[:, at] = (gate * jax.nn.sigmoid(gate) * up).astype(BF)
    h2_ref[...] = (h1.astype(F32) + _dot(act_s[...], wd_ref[...]).astype(BF).astype(F32)).astype(BF)


def ffn(layer, h, o, wo, wg, wu, wd, tb=512, fc=512):
    one = jax.ShapeDtypeStruct((S, D), BF)
    return pl.pallas_call(
        functools.partial(_ffn_kernel, fc=fc), grid=(S // tb,), name="ffn",
        in_specs=[_rows(tb), _rows(tb), _weight(layer, D, D), _weight(layer, D, FF), _weight(layer, D, FF), _weight(layer, FF, D)],
        out_specs=[_rows(tb)] * 2, out_shape=[one] * 2, scratch_shapes=[pltpu.VMEM((tb, FF), BF)],
        compiler_params=_params(48), cost_estimate=_cost(2 * S * D * (D + 3 * FF), 8 * S * D + 6 * D * FF, S * FF),
    )(h, o, wo, wg, wu, wd)


def _ffn_back_kernel(dy_ref, h1_ref, wo_ref, wg_ref, wu_ref, wd_ref, dh1_ref, do_ref, g_ref, dg_s, du_s, ag_s, au_s, ad_s, *, fc, order):
    t = pl.program_id(0)

    @pl.when(t == 0)
    def _():
        for ref in (ag_s, au_s, ad_s):
            ref[...] = jnp.zeros_like(ref)

    dy, h1 = dy_ref[...], h1_ref[...]
    b = _normed(h1)
    bt, dyt = b.T, dy.T
    for c in range(FF // fc):
        at = slice(c * fc, (c + 1) * fc)
        gate, up = _dot(b, wg_ref[:, at]), _dot(b, wu_ref[:, at])
        dact = _dot(dy, wd_ref[at, :], 1, 1).astype(BF).astype(F32)
        sig = jax.nn.sigmoid(gate)
        silu = gate * sig
        act = (silu * up).astype(BF)
        du = (dact * silu).astype(BF)
        dg = (dact * up * (sig + silu * (1 - sig))).astype(BF)
        dg_s[:, at] = dg
        du_s[:, at] = du
        ag_s[:, at] += _dot(bt, dg)
        au_s[:, at] += _dot(bt, du)
        ad_s[:, at] += _dot(dyt, act)
    db = (_dot(dg_s[...], wg_ref[...], 1, 1) + _dot(du_s[...], wu_ref[...], 1, 1)).astype(BF).astype(F32)
    dh1 = (dy.astype(F32) + _norm_back(h1, db).astype(BF).astype(F32)).astype(BF)
    dh1_ref[...] = dh1
    do_ref[...] = _dot(dh1, wo_ref[...], 1, 1).astype(BF)

    @pl.when(t == pl.num_programs(0) - 1)
    def _():
        n = len(order)
        r, f = D // n, FF // n
        for i, to in enumerate(order):
            for c in range(FF // D):
                at = slice(c * D, (c + 1) * D)
                g_ref[to, c * r : (c + 1) * r, :] = ag_s[i * r : (i + 1) * r, at].astype(BF)
                g_ref[to, f + c * r : f + (c + 1) * r, :] = au_s[i * r : (i + 1) * r, at].astype(BF)
            g_ref[to, 2 * f : 3 * f, :] = ad_s[:, i * f : (i + 1) * f].T.astype(BF)


def ffn_back(layer, order, dy, h1, wo, wg, wu, wd, tb=512, fc=512):
    one, n = jax.ShapeDtypeStruct((S, D), BF), len(order)
    return pl.pallas_call(
        functools.partial(_ffn_back_kernel, fc=fc, order=order), grid=(S // tb,), name="ffn_back",
        in_specs=[_rows(tb), _rows(tb), _weight(layer, D, D), _weight(layer, D, FF), _weight(layer, D, FF), _weight(layer, FF, D)],
        out_specs=[_rows(tb), _rows(tb), _whole(n, 3 * FF // n, D)],
        out_shape=[one, one, jax.ShapeDtypeStruct((n, 3 * FF // n, D), BF)],
        scratch_shapes=[pltpu.VMEM((tb, FF), BF)] * 2 + [pltpu.VMEM((D, FF), F32)] * 3,
        compiler_params=_params(63.9), cost_estimate=_cost(2 * S * D * (D + 8 * FF), 8 * S * D + 12 * D * FF, S * FF),
    )(dy, h1, wo, wg, wu, wd)


def _qkv_back_kernel(dq_ref, dk_ref, dv_ref, cos_ref, sin_ref, h_ref, dh1_ref, o_ref, wq_ref, wk_ref, wv_ref, dh_ref, g_ref, acc_s, *, order):
    t = pl.program_id(0)

    @pl.when(t == 0)
    def _():
        acc_s[...] = jnp.zeros_like(acc_s)

    cos, sin = cos_ref[...], sin_ref[...]
    dq, dk, dv = _turn_back(dq_ref[...], cos, sin), _turn_back(dk_ref[...], cos, sin), dv_ref[...]
    h, dh1 = h_ref[...], dh1_ref[...]
    at = _normed(h).T
    acc_s[0] += _dot(at, dq)
    acc_s[1] += _dot(at, dk)
    acc_s[2] += _dot(at, dv)
    acc_s[3] += _dot(o_ref[...].T, dh1)
    if dh_ref is not None:
        da = (_dot(dq, wq_ref[...], 1, 1) + _dot(dk, wk_ref[...], 1, 1) + _dot(dv, wv_ref[...], 1, 1)).astype(BF).astype(F32)
        dh_ref[...] = (dh1.astype(F32) + _norm_back(h, da).astype(BF).astype(F32)).astype(BF)

    @pl.when(t == pl.num_programs(0) - 1)
    def _():
        r = D // len(order)
        for i, to in enumerate(order):
            for c in range(4):
                g_ref[to, c * r : (c + 1) * r, :] = acc_s[c, i * r : (i + 1) * r, :].astype(BF)


def qkv_back(layer, order, dq, dk, dv, cos, sin, h, dh1, o, wq, wk, wv, tb=512):
    w, first, n = _weight(layer, D, D), layer == 0, len(order)
    packed = jax.ShapeDtypeStruct((n, 4 * D // n, D), BF)
    if first:
        def body(*refs, order):
            _qkv_back_kernel(*refs[:8], None, None, None, None, *refs[8:], order=order)
    else:
        body = _qkv_back_kernel
    given = [dq, dk, dv, cos, sin, h, dh1, o] + ([] if first else [wq, wk, wv])
    got = pl.pallas_call(
        functools.partial(body, order=order), grid=(S // tb,), name="qkv_back",
        in_specs=[_rows(tb)] * 3 + [_rows(tb, HALF)] * 2 + [_rows(tb)] * 3 + ([] if first else [w] * 3),
        out_specs=([] if first else [_rows(tb)]) + [_whole(n, 4 * D // n, D)],
        out_shape=([] if first else [jax.ShapeDtypeStruct((S, D), BF)]) + [packed],
        scratch_shapes=[pltpu.VMEM((4, D, D), F32)],
        compiler_params=_params(48), cost_estimate=_cost(2 * S * D * D * (4 if first else 7), 14 * S * D),
    )(*given)
    return (None, got[0]) if first else got


def tables():
    rate = THETA ** (-np.arange(HALF) / HALF)
    low, high = np.arange(128)[:, None] * rate, np.arange(S // 128)[:, None] * 128 * rate
    cl, sl, ch, sh = (jnp.asarray(f(x), F32) for x in (low, high) for f in (np.cos, np.sin))
    cl, sl, ch, sh = cl[None], sl[None], ch[:, None], sh[:, None]
    return (ch * cl - sh * sl).reshape(S, HALF), (sh * cl + ch * sl).reshape(S, HALF)


CHUNK = 128
NZ = 4


def _place():
    me = lax.axis_index("dp")
    core, chip = lax.rem(me, 2), lax.div(me, 2)
    return core, lax.div(chip, NZ), lax.rem(chip, NZ)


def _peer(core, y, z):
    return lax.axis_index("rep"), (y * NZ + z) * 2 + core


def _greet(core, y, z):
    barrier = pltpu.get_barrier_semaphore()
    peers = [_peer(1 - core, y, z), _peer(core, 1 - y, z)] + [_peer(core, y, lax.rem(z + d, NZ)) for d in range(1, NZ)]
    for peer in peers:
        pl.semaphore_signal(barrier, inc=1, device_id=peer, device_id_type=pl.DeviceIdType.MESH)
    pl.semaphore_wait(barrier, len(peers))


def _send(src, dst, send, recv, peer):
    copy = pltpu.make_async_remote_copy(src_ref=src, dst_ref=dst, send_sem=send, recv_sem=recv, device_id=peer, device_id_type=pl.DeviceIdType.MESH)
    copy.start()
    return copy


def _sum_kernel(*refs, pieces, given):
    g_refs, (out_ref, s1, s2, r1, r2, r3, d_send, d_recv, y_send, y_recv, z_send, z_recv) = refs[:given], refs[given:]
    core, y, z = _place()
    _greet(core, y, z)
    count = len(pieces)

    def mine(k):
        which, row = pieces[k]
        return g_refs[which], pl.ds(row, CHUNK)

    first, second, third = [], [], []
    for k in range(count):
        ref, rows = mine(k)
        first.append(_send(ref.at[pl.ds((1 - core) * 8, 8), rows], r1.at[k], d_send.at[k], d_recv.at[k], _peer(1 - core, y, z)))
    for k in range(count):
        ref, rows = mine(k)
        first[k].wait_recv()

        def add(b, _, k=k, ref=ref, rows=rows):
            s1[k, b] = (ref[core * 8 + b, rows, :].astype(F32) + r1[k, b].astype(F32)).astype(BF)
            return _

        lax.fori_loop(0, 8, add, 0)
        second.append(_send(s1.at[k, pl.ds((1 - y) * NZ, NZ)], r2.at[k], y_send.at[k], y_recv.at[k], _peer(core, 1 - y, z)))
    for k in range(count):
        second[k].wait_recv()

        def add(b, _, k=k):
            s2[k, b] = (s1[k, y * NZ + b].astype(F32) + r2[k, b].astype(F32)).astype(BF)
            return _

        lax.fori_loop(0, NZ, add, 0)
        for d in range(1, NZ):
            to = lax.rem(z + d, NZ)
            third.append(_send(s2.at[k, to], r3.at[k, d - 1], z_send.at[k, d - 1], z_recv.at[k, d - 1], _peer(core, y, to)))
    for k in range(count):
        for d in range(NZ - 1):
            third[k * (NZ - 1) + d].wait_recv()
        total = s2[k, z].astype(F32)
        for d in range(NZ - 1):
            total += r3[k, d].astype(F32)
        out_ref[k * CHUNK : (k + 1) * CHUNK, :] = total.astype(BF)
    for copy in first + second + third:
        copy.wait_send()


def sum_blocks(pieces, *packed):
    k = len(pieces)
    vmem = pl.BlockSpec(memory_space=pltpu.VMEM)
    dma = pltpu.SemaphoreType.DMA
    return pl.pallas_call(
        functools.partial(_sum_kernel, pieces=pieces, given=len(packed)), name="sum_blocks",
        in_specs=[vmem] * len(packed), out_specs=vmem, out_shape=jax.ShapeDtypeStruct((k * CHUNK, D), BF),
        scratch_shapes=[pltpu.VMEM((k, m, CHUNK, D), BF) for m in (8, NZ, 8, NZ, NZ - 1)]
        + [dma((k,)), dma((k,)), dma((k,)), dma((k,)), dma((k, NZ - 1)), dma((k, NZ - 1))],
        compiler_params=pltpu.CompilerParams(collective_id=1, has_side_effects=True, vmem_limit_bytes=48 * 2**20),
        cost_estimate=_cost(60e9, 2 * 16 * k * CHUNK * D * 2),
    )(*packed)


def _spread_kernel(*refs, layers, pieces):
    w_refs, late_ref, out_refs = refs[:pieces], refs[pieces], refs[pieces + 1 : 2 * pieces + 1]
    own_sem, late_sem, z_send, z_recv, y_send, y_recv, d_send, d_recv = refs[2 * pieces + 1 :]
    core, y, z = _place()
    at = lambda p, chips: out_refs[p].at[pl.ds(0, layers[p]), chips, core]
    local = [pltpu.make_async_copy(w_refs[p], at(p, y * NZ + z), own_sem.at[p]) for p in range(pieces)]
    r, f = D // 16, FF // 16
    for which in range(2):
        for c in range(FF // D):
            src = late_ref.at[:, :, pl.ds(which * f + c * r, r), :]
            local.append(pltpu.make_async_copy(src, out_refs[4 + which].at[1, :, :, :, pl.ds(c * D, D)], late_sem.at[which * (FF // D) + c]))
    local.append(pltpu.make_async_copy(late_ref.at[:, :, pl.ds(2 * f, f), :], out_refs[6].at[1], late_sem.at[2 * (FF // D)]))
    for copy in local:
        copy.start()
    _greet(core, y, z)
    along, across, over = [], [], []
    for p in range(pieces):
        for d in range(1, NZ):
            along.append(_send(w_refs[p], at(p, y * NZ + z), z_send.at[p, d - 1], z_recv.at[p, d - 1], _peer(core, y, lax.rem(z + d, NZ))))
        across.append([_send(w_refs[p], at(p, y * NZ + z), y_send.at[p, 0], y_recv.at[p, 0], _peer(core, 1 - y, z))])
    for p in range(pieces):
        for d in range(1, NZ):
            along[p * (NZ - 1) + d - 1].wait_recv()
            block = at(p, y * NZ + lax.rem(z + NZ - d, NZ))
            across[p].append(_send(block, block, y_send.at[p, d], y_recv.at[p, d], _peer(core, 1 - y, z)))
        local[p].wait()
        run = at(p, pl.ds(y * NZ, NZ))
        over.append(_send(run, run, d_send.at[p, 0], d_recv.at[p, 0], _peer(1 - core, y, z)))
    for p in range(pieces):
        for copy in across[p]:
            copy.wait_recv()
        run = at(p, pl.ds((1 - y) * NZ, NZ))
        over.append(_send(run, run, d_send.at[p, 1], d_recv.at[p, 1], _peer(1 - core, y, z)))
    for copy in over:
        copy.wait_recv()
    for copy in local[pieces:]:
        copy.wait()
    for copy in along + sum(across, []) + over:
        copy.wait_send()


def spread(given, late):
    k = len(given)
    vmem = pl.BlockSpec(memory_space=pltpu.VMEM)
    dma = pltpu.SemaphoreType.DMA
    late = late.reshape(8, 2, *late.shape[1:])
    return pl.pallas_call(
        functools.partial(_spread_kernel, layers=[w.shape[0] for w in given], pieces=k), name="spread",
        in_specs=[vmem] * k + [pl.BlockSpec(memory_space=pl.ANY)], out_specs=[vmem] * k,
        out_shape=[jax.ShapeDtypeStruct((2, 8, 2, *w.shape[1:]), BF) for w in given],
        scratch_shapes=[dma((k,)), dma((2 * FF // D + 1,)), dma((k, NZ - 1)), dma((k, NZ - 1)), dma((k, NZ)), dma((k, NZ)), dma((k, 2)), dma((k, 2))],
        compiler_params=pltpu.CompilerParams(collective_id=2, has_side_effects=True, vmem_limit_bytes=40 * 2**20),
        cost_estimate=_cost(60e9, 16 * 640 * D * 2),
    )(*given, late)


def adamw(w, m, v, g):
    m = 0.9 * m + 0.1 * g
    v = 0.95 * v + 0.05 * g * g
    step = m * lax.rsqrt(v + 1e-8) + 0.1 * w
    return (w - 0.02 * step).astype(BF), m, v


def _strips(which, n=16):
    r, f = D // n, FF // n
    if which == 2:
        return [(slice(None), slice(0, D), 2 * f)]
    return [(slice(None), slice(c * D, (c + 1) * D), which * f + c * r) for c in range(FF // D)]


def _late_kernel(me_ref, g_ref, *refs):
    w, m, v, (out_ref,) = refs[:3], refs[3:6], refs[6:9], refs[9:]
    for i in range(3):
        for rows, cols, at in _strips(i):
            here = slice(at, at + w[i].shape[0])
            new, _, _ = adamw(w[i][rows, cols].astype(F32), m[i][rows, cols], v[i][rows, cols], g_ref[here, :].astype(F32))
            out_ref[here, :] = new


def late_weights(me, g, w, m, v):
    block = lambda a, own: pl.BlockSpec((None, a.shape[1], a.shape[2]), (lambda i, me: (1, me[0], 0)) if own else (lambda i, me: (1, 0, 0)))
    cut = lambda a, like: pl.BlockSpec((None, like.shape[1], like.shape[2]), lambda i, me: (1, me[0], 0))
    return pl.pallas_call(
        _late_kernel, name="late_weights", out_shape=jax.ShapeDtypeStruct(g.shape, BF),
        grid_spec=pltpu.PrefetchScalarGridSpec(
            num_scalar_prefetch=1, grid=(1,),
            in_specs=[pl.BlockSpec(g.shape, lambda i, me: (0, 0))] + [cut(a, b) for a, b in zip(w, m)] + [block(a, False) for a in (*m, *v)],
            out_specs=pl.BlockSpec(g.shape, lambda i, me: (0, 0))),
        compiler_params=_params(16), cost_estimate=_cost(2e9, 5e6),
    )(me, g, *w, *m, *v)


def _update_kernel(me_ref, got_ref, late_ref, *refs):
    w, m, v = refs[:7], refs[7:14], refs[14:21]
    new_w, new_m, new_v = refs[21:28], refs[28:35], refs[35:42]
    r = D // 16
    for i in range(4):
        for layer, first in ((0, 512), (1, 0)):
            g = got_ref[first + i * r : first + (i + 1) * r, :].astype(F32)
            new_w[i][layer], new_m[i][layer], new_v[i][layer] = adamw(w[i][layer].astype(F32), m[i][layer], v[i][layer], g)
    for i in range(3):
        for rows, cols, at in _strips(i):
            for layer, ref, first in ((0, got_ref, 128), (1, late_ref, 0)):
                here = (layer, rows, cols)
                g = ref[first + at : first + at + m[4 + i].shape[1], :].astype(F32)
                a, b, c = adamw(w[4 + i][here].astype(F32), m[4 + i][here], v[4 + i][here], g)
                new_m[4 + i][here], new_v[4 + i][here] = b, c
                if layer == 0:
                    new_w[4 + i][here] = a


def update(me, got, late, w, m, v):
    full = lambda a: pl.BlockSpec(a.shape, lambda i, me: (0,) * len(a.shape))
    cut = lambda like: pl.BlockSpec(like.shape, lambda i, me: (0, me[0], 0))
    shape = lambda a, t, layers=2: jax.ShapeDtypeStruct((layers, *a.shape[1:]), t)
    outs = [shape(a, BF, 2 if i < 4 else 1) for i, a in enumerate(m)] + [shape(a, F32) for a in (*m, *v)]
    out = pl.pallas_call(
        _update_kernel, name="update", out_shape=outs,
        grid_spec=pltpu.PrefetchScalarGridSpec(
            num_scalar_prefetch=1, grid=(1,),
            in_specs=[full(got), full(late)] + [cut(a) for a in m] + [full(a) for a in (*m, *v)],
            out_specs=[full(a) for a in outs]),
        compiler_params=_params(40), cost_estimate=_cost(2e9, 12e6),
    )(me, got, late, *w, *m, *v)
    return out[:7], out[7:14], out[14:]


def solution(mesh):
    n = mesh.shape["dp"]
    plain = tuple(range(n))
    order = tuple((i % 2) * (n // 2) + i // 2 for i in range(n))

    def step(x, dy, wq, wk, wv, wo, wg, wu, wd, *moments):
        weights, m, v = (wq, wk, wv, wo, wg, wu, wd), moments[:7], moments[7:]
        me = lax.axis_index("dp").reshape(1)
        cos, sin = tables()
        h0 = x[0]
        q0, k0, v0 = qkv(0, h0, cos, sin, wq, wk, wv)
        o0, l0 = attend(q0, k0, v0)
        m0, h1 = ffn(0, h0, o0, wo, wg, wu, wd)
        q1, k1, v1 = qkv(1, h1, cos, sin, wq, wk, wv)
        o1, l1 = attend(q1, k1, v1)
        m1 = project(1, h1, o1, wo)
        dm1, do1, gf1 = ffn_back(1, plain, dy[0], m1, wo, wg, wu, wd)
        gf1 = lax.psum_scatter(gf1, "dp", scatter_dimension=0, tiled=False)
        dq1, dk1, dv1 = attend_back(q1, k1, v1, o1, do1, l1)
        dh1, ga1 = qkv_back(1, order, dq1, dk1, dv1, cos, sin, h1, dm1, o1, wq, wk, wv)
        dm0, do0, gf0 = ffn_back(0, order, dh1, m0, wo, wg, wu, wd)
        do0, gf1 = lax.optimization_barrier((do0, gf1))
        late = late_weights(me, gf1, weights[4:], m[4:], v[4:])
        all_late = lax.all_gather(late, "dp", axis=0, tiled=False)
        dq0, dk0, dv0 = attend_back(q0, k0, v0, o0, do0, l0)
        _, ga0 = qkv_back(0, order, dq0, dk0, dv0, cos, sin, h0, dm0, o0, wq, wk, wv)
        ga0, _ = lax.optimization_barrier((ga0, late))
        got = sum_blocks(((0, 0), (1, 0), (1, 128), (1, 256), (2, 0)), ga1, gf0, ga0)
        new, new_m, new_v = update(me, got, gf1, weights, m, v)
        out = spread(new, all_late)
        return (*(a.reshape(w.shape) for a, w in zip(out, weights)), *new_m, *new_v)

    states, all_of, cut = P(("rep", "dp"), None, None), P(None, None, None), P(None, "dp", None)
    return jax.shard_map(
        step, mesh=mesh, in_specs=(states, states) + (all_of,) * 7 + (cut,) * 14,
        out_specs=(P("rep", None, None),) * 7 + (P("rep", "dp", None),) * 14, check_vma=False,
    )
```

```python
import functools

import jax
import jax.numpy as jnp
import numpy as np
from jax import lax
from jax.experimental import pallas as pl
from jax.experimental.pallas import tpu as pltpu
from jax.sharding import PartitionSpec as P

LOG2E = 1.4426950408889634
BF, F32 = jnp.bfloat16, jnp.float32
D, HEAD, HEADS, FF, S = 512, 256, 2, 2048, 2048
HALF = HEAD // 2
THETA = 10000
STRIP = 512
N_STRIP = S // STRIP
E = HEAD**-0.5 * LOG2E
HIDDEN = -2e30


def _dot(a, b, ca=1, cb=0):
    return lax.dot_general(a, b, (((ca,), (cb,)), ((), ())), preferred_element_type=F32)


def _scale_of(wide):
    return lax.rsqrt(jnp.mean(wide * wide, -1, keepdims=True) + 1e-6)


def _normed(h):
    wide = h.astype(F32)
    return (wide * _scale_of(wide)).astype(BF)


def _norm_back(h, ct):
    wide = h.astype(F32)
    scale = _scale_of(wide)
    return ct * scale - wide * (scale * scale * scale * jnp.mean(ct * wide, -1, keepdims=True))


def _params(vmem, grid=1):
    return pltpu.CompilerParams(dimension_semantics=("arbitrary",) * grid, vmem_limit_bytes=int(vmem * 2**20))


def _cost(flops, nbytes, trans=0):
    return pl.CostEstimate(flops=int(flops), bytes_accessed=int(nbytes), transcendentals=int(trans))


def _rows(tb, width=D):
    return pl.BlockSpec((tb, width), lambda t: (t, 0))


def _weight(layer, *shape):
    return pl.BlockSpec((None, *shape), lambda *_: (layer, 0, 0))


def _whole(*shape):
    return pl.BlockSpec(shape, lambda *_: (0,) * len(shape))


def _turn(t, cos, sin):
    out = []
    for i in range(HEADS):
        a = t[:, i * HEAD : i * HEAD + HALF].astype(F32)
        b = t[:, i * HEAD + HALF : (i + 1) * HEAD].astype(F32)
        out += [a * cos - b * sin, b * cos + a * sin]
    return jnp.concatenate(out, -1).astype(BF)


def _turn_back(t, cos, sin):
    out = []
    for i in range(HEADS):
        a = t[:, i * HEAD : i * HEAD + HALF].astype(F32)
        b = t[:, i * HEAD + HALF : (i + 1) * HEAD].astype(F32)
        out += [a * cos + b * sin, b * cos - a * sin]
    return jnp.concatenate(out, -1).astype(BF)


def _qkv_kernel(h_ref, cos_ref, sin_ref, wq_ref, wk_ref, wv_ref, q_ref, k_ref, v_ref):
    a = _normed(h_ref[...])
    cos, sin = cos_ref[...], sin_ref[...]
    q_ref[...] = _turn(_dot(a, wq_ref[...]).astype(BF), cos, sin)
    k_ref[...] = _turn(_dot(a, wk_ref[...]).astype(BF), cos, sin)
    v_ref[...] = _dot(a, wv_ref[...]).astype(BF)


def qkv(layer, h, cos, sin, wq, wk, wv, tb=512):
    one = jax.ShapeDtypeStruct((S, D), BF)
    w = _weight(layer, D, D)
    return pl.pallas_call(
        _qkv_kernel, grid=(S // tb,), name="qkv",
        in_specs=[_rows(tb), _rows(tb, HALF), _rows(tb, HALF), w, w, w],
        out_specs=[_rows(tb)] * 3, out_shape=[one] * 3,
        compiler_params=_params(14), cost_estimate=_cost(3 * 2 * S * D * D, 4 * S * D * 2 + 2 * S * HALF * 4),
    )(h, cos, sin, wq, wk, wv)


def _diag():
    shape = (STRIP, STRIP)
    return lax.broadcasted_iota(jnp.int32, shape, 1) >= lax.broadcasted_iota(jnp.int32, shape, 0)


def _attend_kernel(q_ref, k_ref, v_ref, o_ref, lse_ref, vt_s, sc_s, p_s):
    ok = _diag()
    for i in range(HEADS):
        col = slice(i * HEAD, (i + 1) * HEAD)
        vt_s[i, :HEAD, :] = v_ref[:, col].T
        vt_s[i, HEAD:, :] = jnp.ones((16, S), BF)
    for s in range(N_STRIP):
        for i in range(HEADS):
            col = slice(i * HEAD, (i + 1) * HEAD)
            here = slice(s * STRIP, (s + 1) * STRIP)
            n = (s + 1) * STRIP
            q = q_ref[here, col]
            top = None
            for j in range(s + 1):
                sc = _dot(k_ref[j * STRIP : (j + 1) * STRIP, col], q, 1, 1)
                if j == s:
                    sc = jnp.where(ok, sc, HIDDEN)
                sc_s[i, j * STRIP : (j + 1) * STRIP, :] = sc
                m = sc.max(axis=0, keepdims=True)
                top = m if top is None else jnp.maximum(top, m)
            for j in range(s + 1):
                at = slice(j * STRIP, (j + 1) * STRIP)
                p_s[i, at, :] = jnp.exp2((sc_s[i, at, :] - top) * E).astype(BF)
            mix = _dot(vt_s[i, :, :n], p_s[i, :n, :])
            total = mix[HEAD : HEAD + 1, :]
            o_ref[here, col] = (mix[:HEAD, :] * (1 / total)).T.astype(BF)
            lse_ref[i : i + 1, here] = top * (HEAD**-0.5) + jnp.log(total)


def attend(q, k, v):
    return pl.pallas_call(
        _attend_kernel, grid=(1,), name="attend",
        in_specs=[_whole(S, D)] * 3, out_specs=[_whole(S, D), _whole(8, S)],
        out_shape=[jax.ShapeDtypeStruct((S, D), BF), jax.ShapeDtypeStruct((8, S), F32)],
        scratch_shapes=[pltpu.VMEM((HEADS, HEAD + 16, S), BF), pltpu.VMEM((HEADS, S, STRIP), F32), pltpu.VMEM((HEADS, S, STRIP), BF)],
        compiler_params=_params(30), cost_estimate=_cost(2 * HEADS * S * S * HEAD * 1.25, 8 * S * D, HEADS * S * S * 0.6),
    )(q, k, v)


def _attend_back_kernel(q_ref, k_ref, v_ref, o_ref, do_ref, lse_ref, dq_ref, dk_ref, dv_ref, dq_s, p_s, ds_s):
    ok = _diag()
    for i in range(HEADS):
        col = slice(i * HEAD, (i + 1) * HEAD)
        lse = lse_ref[i : i + 1, :] * LOG2E
        deltas = []
        for s in range(N_STRIP):
            here = slice(s * STRIP, (s + 1) * STRIP)
            both = do_ref[here, col].astype(F32) * o_ref[here, col].astype(F32)
            delta = both.sum(-1, keepdims=True)
            deltas.append(jnp.broadcast_to(delta, (STRIP, 128)).T[0:1, :])
        for j in range(N_STRIP):
            at = slice(j * STRIP, (j + 1) * STRIP)
            k, v = k_ref[at, col], v_ref[at, col]
            kt = k.T
            for s in range(j, N_STRIP):
                here = slice(s * STRIP, (s + 1) * STRIP)
                p = jnp.exp2(_dot(k, q_ref[here, col], 1, 1) * E - lse[:, here])
                if s == j:
                    p = jnp.where(ok, p, 0.0)
                dp = _dot(v, do_ref[here, col], 1, 1)
                ds = (p * (dp - deltas[s])).astype(BF)
                p_s[i, :, here] = p.astype(BF)
                ds_s[i, :, here] = ds
                part = _dot(kt, ds)
                if j == 0:
                    dq_s[i, :, here] = part
                else:
                    dq_s[i, :, here] += part
            rest = slice(j * STRIP, S)
            dv_ref[at, col] = _dot(p_s[i, :, rest], do_ref[rest, col]).astype(BF)
            dk_ref[at, col] = (_dot(ds_s[i, :, rest], q_ref[rest, col]) * (HEAD**-0.5)).astype(BF)
        dq_ref[:, col] = (dq_s[i] * (HEAD**-0.5)).T.astype(BF)


def attend_back(q, k, v, o, do, lse):
    one = jax.ShapeDtypeStruct((S, D), BF)
    return pl.pallas_call(
        _attend_back_kernel, grid=(1,), name="attend_back",
        in_specs=[_whole(S, D)] * 5 + [_whole(8, S)], out_specs=[_whole(S, D)] * 3, out_shape=[one] * 3,
        scratch_shapes=[pltpu.VMEM((HEADS, HEAD, S), F32), pltpu.VMEM((HEADS, STRIP, S), BF), pltpu.VMEM((HEADS, STRIP, S), BF)],
        compiler_params=_params(44), cost_estimate=_cost(5 * HEADS * S * S * HEAD * 1.25, 16 * S * D, HEADS * S * S * 0.6),
    )(q, k, v, o, do, lse)


def _project_kernel(h_ref, o_ref, wo_ref, h1_ref):
    h1_ref[...] = (h_ref[...].astype(F32) + _dot(o_ref[...], wo_ref[...]).astype(BF).astype(F32)).astype(BF)


def project(layer, h, o, wo, tb=512):
    return pl.pallas_call(
        _project_kernel, grid=(S // tb,), name="project",
        in_specs=[_rows(tb), _rows(tb), _weight(layer, D, D)], out_specs=_rows(tb), out_shape=jax.ShapeDtypeStruct((S, D), BF),
        compiler_params=_params(8), cost_estimate=_cost(2 * S * D * D, 6 * S * D),
    )(h, o, wo)


def _ffn_kernel(h_ref, o_ref, wo_ref, wg_ref, wu_ref, wd_ref, h1_ref, h2_ref, act_s, *, fc):
    h1 = (h_ref[...].astype(F32) + _dot(o_ref[...], wo_ref[...]).astype(BF).astype(F32)).astype(BF)
    h1_ref[...] = h1
    b = _normed(h1)
    for c in range(FF // fc):
        at = slice(c * fc, (c + 1) * fc)
        gate, up = _dot(b, wg_ref[:, at]), _dot(b, wu_ref[:, at])
        act_s[:, at] = (gate * jax.nn.sigmoid(gate) * up).astype(BF)
    h2_ref[...] = (h1.astype(F32) + _dot(act_s[...], wd_ref[...]).astype(BF).astype(F32)).astype(BF)


def ffn(layer, h, o, wo, wg, wu, wd, tb=512, fc=512):
    one = jax.ShapeDtypeStruct((S, D), BF)
    return pl.pallas_call(
        functools.partial(_ffn_kernel, fc=fc), grid=(S // tb,), name="ffn",
        in_specs=[_rows(tb), _rows(tb), _weight(layer, D, D), _weight(layer, D, FF), _weight(layer, D, FF), _weight(layer, FF, D)],
        out_specs=[_rows(tb)] * 2, out_shape=[one] * 2, scratch_shapes=[pltpu.VMEM((tb, FF), BF)],
        compiler_params=_params(26), cost_estimate=_cost(2 * S * D * (D + 3 * FF), 8 * S * D + 6 * D * FF, S * FF),
    )(h, o, wo, wg, wu, wd)


def _ffn_back_kernel(dy_ref, h1_ref, wo_ref, wg_ref, wu_ref, wd_ref, dh1_ref, do_ref, g_ref, dg_s, du_s, ag_s, au_s, ad_s, *, fc, order):
    t = pl.program_id(0)

    @pl.when(t == 0)
    def _():
        for ref in (ag_s, au_s, ad_s):
            ref[...] = jnp.zeros_like(ref)

    dy, h1 = dy_ref[...], h1_ref[...]
    b = _normed(h1)
    bt, dyt = b.T, dy.T
    for c in range(FF // fc):
        at = slice(c * fc, (c + 1) * fc)
        gate, up = _dot(b, wg_ref[:, at]), _dot(b, wu_ref[:, at])
        dact = _dot(dy, wd_ref[at, :], 1, 1).astype(BF).astype(F32)
        sig = jax.nn.sigmoid(gate)
        silu = gate * sig
        act = (silu * up).astype(BF)
        du = (dact * silu).astype(BF)
        dg = (dact * up * (sig + silu * (1 - sig))).astype(BF)
        dg_s[:, at] = dg
        du_s[:, at] = du
        ag_s[:, at] += _dot(bt, dg)
        au_s[:, at] += _dot(bt, du)
        ad_s[:, at] += _dot(dyt, act)
    db = (_dot(dg_s[...], wg_ref[...], 1, 1) + _dot(du_s[...], wu_ref[...], 1, 1)).astype(BF).astype(F32)
    dh1 = (dy.astype(F32) + _norm_back(h1, db).astype(BF).astype(F32)).astype(BF)
    dh1_ref[...] = dh1
    do_ref[...] = _dot(dh1, wo_ref[...], 1, 1).astype(BF)

    @pl.when(t == pl.num_programs(0) - 1)
    def _():
        n = len(order)
        r, f = D // n, FF // n
        for i, to in enumerate(order):
            for c in range(FF // D):
                at = slice(c * D, (c + 1) * D)
                g_ref[to, c * r : (c + 1) * r, :] = ag_s[i * r : (i + 1) * r, at].astype(BF)
                g_ref[to, f + c * r : f + (c + 1) * r, :] = au_s[i * r : (i + 1) * r, at].astype(BF)
            g_ref[to, 2 * f : 3 * f, :] = ad_s[:, i * f : (i + 1) * f].T.astype(BF)


def ffn_back(layer, order, dy, h1, wo, wg, wu, wd, tb=512, fc=512):
    one, n = jax.ShapeDtypeStruct((S, D), BF), len(order)
    return pl.pallas_call(
        functools.partial(_ffn_back_kernel, fc=fc, order=order), grid=(S // tb,), name="ffn_back",
        in_specs=[_rows(tb), _rows(tb), _weight(layer, D, D), _weight(layer, D, FF), _weight(layer, D, FF), _weight(layer, FF, D)],
        out_specs=[_rows(tb), _rows(tb), _whole(n, 3 * FF // n, D)],
        out_shape=[one, one, jax.ShapeDtypeStruct((n, 3 * FF // n, D), BF)],
        scratch_shapes=[pltpu.VMEM((tb, FF), BF)] * 2 + [pltpu.VMEM((D, FF), F32)] * 3,
        compiler_params=_params(63.9), cost_estimate=_cost(2 * S * D * (D + 8 * FF), 8 * S * D + 12 * D * FF, S * FF),
    )(dy, h1, wo, wg, wu, wd)


def _qkv_back_kernel(dq_ref, dk_ref, dv_ref, cos_ref, sin_ref, h_ref, dh1_ref, o_ref, wq_ref, wk_ref, wv_ref, dh_ref, g_ref, acc_s, *, order):
    t = pl.program_id(0)

    @pl.when(t == 0)
    def _():
        acc_s[...] = jnp.zeros_like(acc_s)

    cos, sin = cos_ref[...], sin_ref[...]
    dq, dk, dv = _turn_back(dq_ref[...], cos, sin), _turn_back(dk_ref[...], cos, sin), dv_ref[...]
    h, dh1 = h_ref[...], dh1_ref[...]
    at = _normed(h).T
    acc_s[0] += _dot(at, dq)
    acc_s[1] += _dot(at, dk)
    acc_s[2] += _dot(at, dv)
    acc_s[3] += _dot(o_ref[...].T, dh1)
    if dh_ref is not None:
        da = (_dot(dq, wq_ref[...], 1, 1) + _dot(dk, wk_ref[...], 1, 1) + _dot(dv, wv_ref[...], 1, 1)).astype(BF).astype(F32)
        dh_ref[...] = (dh1.astype(F32) + _norm_back(h, da).astype(BF).astype(F32)).astype(BF)

    @pl.when(t == pl.num_programs(0) - 1)
    def _():
        r = D // len(order)
        for i, to in enumerate(order):
            for c in range(4):
                g_ref[to, c * r : (c + 1) * r, :] = acc_s[c, i * r : (i + 1) * r, :].astype(BF)


def qkv_back(layer, order, dq, dk, dv, cos, sin, h, dh1, o, wq, wk, wv, tb=512):
    w, first, n = _weight(layer, D, D), layer == 0, len(order)
    packed = jax.ShapeDtypeStruct((n, 4 * D // n, D), BF)
    if first:
        def body(*refs, order):
            _qkv_back_kernel(*refs[:8], None, None, None, None, *refs[8:], order=order)
    else:
        body = _qkv_back_kernel
    given = [dq, dk, dv, cos, sin, h, dh1, o] + ([] if first else [wq, wk, wv])
    got = pl.pallas_call(
        functools.partial(body, order=order), grid=(S // tb,), name="qkv_back",
        in_specs=[_rows(tb)] * 3 + [_rows(tb, HALF)] * 2 + [_rows(tb)] * 3 + ([] if first else [w] * 3),
        out_specs=([] if first else [_rows(tb)]) + [_whole(n, 4 * D // n, D)],
        out_shape=([] if first else [jax.ShapeDtypeStruct((S, D), BF)]) + [packed],
        scratch_shapes=[pltpu.VMEM((4, D, D), F32)],
        compiler_params=_params(24), cost_estimate=_cost(2 * S * D * D * (4 if first else 7), 14 * S * D),
    )(*given)
    return (None, got[0]) if first else got


def tables():
    rate = THETA ** (-np.arange(HALF) / HALF)
    low, high = np.arange(128)[:, None] * rate, np.arange(S // 128)[:, None] * 128 * rate
    cl, sl, ch, sh = (jnp.asarray(f(x), F32) for x in (low, high) for f in (np.cos, np.sin))
    cl, sl, ch, sh = cl[None], sl[None], ch[:, None], sh[:, None]
    return (ch * cl - sh * sl).reshape(S, HALF), (sh * cl + ch * sl).reshape(S, HALF)


CHUNK = 128
NZ = 4


def _place():
    me = lax.axis_index("dp")
    core, chip = lax.rem(me, 2), lax.div(me, 2)
    return core, lax.div(chip, NZ), lax.rem(chip, NZ)


def _peer(core, y, z):
    return lax.axis_index("rep"), (y * NZ + z) * 2 + core


def _greet(core, y, z):
    barrier = pltpu.get_barrier_semaphore()
    peers = [_peer(1 - core, y, z), _peer(core, 1 - y, z)] + [_peer(core, y, lax.rem(z + d, NZ)) for d in range(1, NZ)]
    for peer in peers:
        pl.semaphore_signal(barrier, inc=1, device_id=peer, device_id_type=pl.DeviceIdType.MESH)
    pl.semaphore_wait(barrier, len(peers))


def _send(src, dst, send, recv, peer):
    copy = pltpu.make_async_remote_copy(src_ref=src, dst_ref=dst, send_sem=send, recv_sem=recv, device_id=peer, device_id_type=pl.DeviceIdType.MESH)
    copy.start()
    return copy


def _sum_kernel(*refs, pieces, given):
    g_refs, (out_ref, own, s1, s2, r1, r2, r3, own_sem, d_send, d_recv, y_send, y_recv, z_send, z_recv) = refs[:given], refs[given:]
    core, y, z = _place()
    count = len(pieces)

    def mine(k):
        which, row = pieces[k]
        return g_refs[which], pl.ds(row, CHUNK)

    first, second, third, local = [], [], [], []
    for k in range(count):
        ref, rows = mine(k)
        local.append(pltpu.make_async_copy(ref.at[pl.ds(core * 8, 8), rows], own.at[k], own_sem.at[k]))
        local[k].start()
    _greet(core, y, z)
    for k in range(count):
        ref, rows = mine(k)
        first.append(_send(ref.at[pl.ds((1 - core) * 8, 8), rows], r1.at[k], d_send.at[k], d_recv.at[k], _peer(1 - core, y, z)))
    for k in range(count):
        local[k].wait()
        first[k].wait_recv()

        def add(b, _, k=k):
            s1[k, b] = (own[k, b].astype(F32) + r1[k, b].astype(F32)).astype(BF)
            return _

        lax.fori_loop(0, 8, add, 0)
        second.append(_send(s1.at[k, pl.ds((1 - y) * NZ, NZ)], r2.at[k], y_send.at[k], y_recv.at[k], _peer(core, 1 - y, z)))
    for k in range(count):
        second[k].wait_recv()

        def add(b, _, k=k):
            s2[k, b] = (s1[k, y * NZ + b].astype(F32) + r2[k, b].astype(F32)).astype(BF)
            return _

        lax.fori_loop(0, NZ, add, 0)
        for d in range(1, NZ):
            to = lax.rem(z + d, NZ)
            third.append(_send(s2.at[k, to], r3.at[k, d - 1], z_send.at[k, d - 1], z_recv.at[k, d - 1], _peer(core, y, to)))
    for k in range(count):
        for d in range(NZ - 1):
            third[k * (NZ - 1) + d].wait_recv()
        total = s2[k, z].astype(F32)
        for d in range(NZ - 1):
            total += r3[k, d].astype(F32)
        out_ref[k * CHUNK : (k + 1) * CHUNK, :] = total.astype(BF)
    for copy in first + second + third:
        copy.wait_send()


def sum_blocks(pieces, *packed):
    k = len(pieces)
    vmem = pl.BlockSpec(memory_space=pltpu.VMEM)
    dma = pltpu.SemaphoreType.DMA
    return pl.pallas_call(
        functools.partial(_sum_kernel, pieces=pieces, given=len(packed)), name="sum_blocks",
        in_specs=[pl.BlockSpec(memory_space=pl.ANY)] * len(packed), out_specs=vmem, out_shape=jax.ShapeDtypeStruct((k * CHUNK, D), BF),
        scratch_shapes=[pltpu.VMEM((k, m, CHUNK, D), BF) for m in (8, 8, NZ, 8, NZ, NZ - 1)]
        + [dma((k,)), dma((k,)), dma((k,)), dma((k,)), dma((k,)), dma((k, NZ - 1)), dma((k, NZ - 1))],
        compiler_params=pltpu.CompilerParams(collective_id=1, has_side_effects=True, vmem_limit_bytes=60 * 2**20),
        cost_estimate=_cost(60e9, 2 * 16 * k * CHUNK * D * 2),
    )(*packed)


def _spread_kernel(*refs, layers, pieces):
    w_refs, late_ref, out_refs = refs[:pieces], refs[pieces], refs[pieces + 1 : 2 * pieces + 1]
    own_sem, late_sem, z_send, z_recv, y_send, y_recv, d_send, d_recv = refs[2 * pieces + 1 :]
    core, y, z = _place()
    at = lambda p, chips: out_refs[p].at[pl.ds(0, layers[p]), chips, core]
    local = [pltpu.make_async_copy(w_refs[p], at(p, y * NZ + z), own_sem.at[p]) for p in range(pieces)]
    r, f = D // 16, FF // 16
    for which in range(2):
        for c in range(FF // D):
            src = late_ref.at[:, :, pl.ds(which * f + c * r, r), :]
            local.append(pltpu.make_async_copy(src, out_refs[4 + which].at[1, :, :, :, pl.ds(c * D, D)], late_sem.at[which * (FF // D) + c]))
    local.append(pltpu.make_async_copy(late_ref.at[:, :, pl.ds(2 * f, f), :], out_refs[6].at[1], late_sem.at[2 * (FF // D)]))
    for copy in local:
        copy.start()
    _greet(core, y, z)
    along, across, over = [], [], []
    for p in range(pieces):
        for d in range(1, NZ):
            along.append(_send(w_refs[p], at(p, y * NZ + z), z_send.at[p, d - 1], z_recv.at[p, d - 1], _peer(core, y, lax.rem(z + d, NZ))))
        across.append([_send(w_refs[p], at(p, y * NZ + z), y_send.at[p, 0], y_recv.at[p, 0], _peer(core, 1 - y, z))])
    for p in range(pieces):
        for d in range(1, NZ):
            along[p * (NZ - 1) + d - 1].wait_recv()
            block = at(p, y * NZ + lax.rem(z + NZ - d, NZ))
            across[p].append(_send(block, block, y_send.at[p, d], y_recv.at[p, d], _peer(core, 1 - y, z)))
        local[p].wait()
        run = at(p, pl.ds(y * NZ, NZ))
        over.append(_send(run, run, d_send.at[p, 0], d_recv.at[p, 0], _peer(1 - core, y, z)))
    for p in range(pieces):
        for copy in across[p]:
            copy.wait_recv()
        run = at(p, pl.ds((1 - y) * NZ, NZ))
        over.append(_send(run, run, d_send.at[p, 1], d_recv.at[p, 1], _peer(1 - core, y, z)))
    for copy in over:
        copy.wait_recv()
    for copy in local[pieces:]:
        copy.wait()
    for copy in along + sum(across, []) + over:
        copy.wait_send()


def spread(given, late):
    k = len(given)
    vmem = pl.BlockSpec(memory_space=pltpu.VMEM)
    dma = pltpu.SemaphoreType.DMA
    late = late.reshape(8, 2, *late.shape[1:])
    return pl.pallas_call(
        functools.partial(_spread_kernel, layers=[w.shape[0] for w in given], pieces=k), name="spread",
        in_specs=[vmem] * k + [pl.BlockSpec(memory_space=pl.ANY)], out_specs=[vmem] * k,
        out_shape=[jax.ShapeDtypeStruct((2, 8, 2, *w.shape[1:]), BF) for w in given],
        scratch_shapes=[dma((k,)), dma((2 * FF // D + 1,)), dma((k, NZ - 1)), dma((k, NZ - 1)), dma((k, NZ)), dma((k, NZ)), dma((k, 2)), dma((k, 2))],
        compiler_params=pltpu.CompilerParams(collective_id=2, has_side_effects=True, vmem_limit_bytes=40 * 2**20),
        cost_estimate=_cost(60e9, 16 * 640 * D * 2),
    )(*given, late)


def adamw(w, m, v, g):
    m = 0.9 * m + 0.1 * g
    v = 0.95 * v + 0.05 * g * g
    step = m * lax.rsqrt(v + 1e-8) + 0.1 * w
    return (w - 0.02 * step).astype(BF), m, v


def _strips(which, n=16):
    r, f = D // n, FF // n
    if which == 2:
        return [(slice(None), slice(0, D), 2 * f)]
    return [(slice(None), slice(c * D, (c + 1) * D), which * f + c * r) for c in range(FF // D)]


def _late_kernel(me_ref, g_ref, *refs):
    w, m, v, (out_ref,) = refs[:3], refs[3:6], refs[6:9], refs[9:]
    for i in range(3):
        for rows, cols, at in _strips(i):
            here = slice(at, at + w[i].shape[0])
            new, _, _ = adamw(w[i][rows, cols].astype(F32), m[i][rows, cols], v[i][rows, cols], g_ref[here, :].astype(F32))
            out_ref[here, :] = new


def late_weights(me, g, w, m, v):
    block = lambda a, own: pl.BlockSpec((None, a.shape[1], a.shape[2]), (lambda i, me: (1, me[0], 0)) if own else (lambda i, me: (1, 0, 0)))
    cut = lambda a, like: pl.BlockSpec((None, like.shape[1], like.shape[2]), lambda i, me: (1, me[0], 0))
    return pl.pallas_call(
        _late_kernel, name="late_weights", out_shape=jax.ShapeDtypeStruct(g.shape, BF),
        grid_spec=pltpu.PrefetchScalarGridSpec(
            num_scalar_prefetch=1, grid=(1,),
            in_specs=[pl.BlockSpec(g.shape, lambda i, me: (0, 0))] + [cut(a, b) for a, b in zip(w, m)] + [block(a, False) for a in (*m, *v)],
            out_specs=pl.BlockSpec(g.shape, lambda i, me: (0, 0))),
        compiler_params=_params(60), cost_estimate=_cost(2e9, 5e6),
    )(me, g, *w, *m, *v)


def _update_kernel(me_ref, got_ref, late_ref, *refs):
    w, m, v = refs[:7], refs[7:14], refs[14:21]
    new_w, new_m, new_v = refs[21:28], refs[28:35], refs[35:42]
    r = D // 16
    for i in range(4):
        for layer, first in ((0, 512), (1, 0)):
            g = got_ref[first + i * r : first + (i + 1) * r, :].astype(F32)
            new_w[i][layer], new_m[i][layer], new_v[i][layer] = adamw(w[i][layer].astype(F32), m[i][layer], v[i][layer], g)
    for i in range(3):
        for rows, cols, at in _strips(i):
            for layer, ref, first in ((0, got_ref, 128), (1, late_ref, 0)):
                here = (layer, rows, cols)
                g = ref[first + at : first + at + m[4 + i].shape[1], :].astype(F32)
                a, b, c = adamw(w[4 + i][here].astype(F32), m[4 + i][here], v[4 + i][here], g)
                new_m[4 + i][here], new_v[4 + i][here] = b, c
                if layer == 0:
                    new_w[4 + i][here] = a


def update(me, got, late, w, m, v):
    full = lambda a: pl.BlockSpec(a.shape, lambda i, me: (0,) * len(a.shape))
    cut = lambda like: pl.BlockSpec(like.shape, lambda i, me: (0, me[0], 0))
    shape = lambda a, t, layers=2: jax.ShapeDtypeStruct((layers, *a.shape[1:]), t)
    outs = [shape(a, BF, 2 if i < 4 else 1) for i, a in enumerate(m)] + [shape(a, F32) for a in (*m, *v)]
    out = pl.pallas_call(
        _update_kernel, name="update", out_shape=outs,
        grid_spec=pltpu.PrefetchScalarGridSpec(
            num_scalar_prefetch=1, grid=(1,),
            in_specs=[full(got), full(late)] + [cut(a) for a in m] + [full(a) for a in (*m, *v)],
            out_specs=[full(a) for a in outs]),
        compiler_params=_params(60), cost_estimate=_cost(2e9, 12e6),
    )(me, got, late, *w, *m, *v)
    return out[:7], out[7:14], out[14:]


def solution(mesh):
    n = mesh.shape["dp"]
    plain = tuple(range(n))
    order = tuple((i % 2) * (n // 2) + i // 2 for i in range(n))

    def step(x, dy, wq, wk, wv, wo, wg, wu, wd, *moments):
        weights, m, v = (wq, wk, wv, wo, wg, wu, wd), moments[:7], moments[7:]
        me = lax.axis_index("dp").reshape(1)
        cos, sin = tables()
        h0 = x[0]
        q0, k0, v0 = qkv(0, h0, cos, sin, wq, wk, wv)
        o0, l0 = attend(q0, k0, v0)
        m0, h1 = ffn(0, h0, o0, wo, wg, wu, wd)
        q1, k1, v1 = qkv(1, h1, cos, sin, wq, wk, wv)
        o1, l1 = attend(q1, k1, v1)
        m1 = project(1, h1, o1, wo)
        dm1, do1, gf1 = ffn_back(1, plain, dy[0], m1, wo, wg, wu, wd)
        gf1 = lax.psum_scatter(gf1, "dp", scatter_dimension=0, tiled=False)
        dq1, dk1, dv1 = attend_back(q1, k1, v1, o1, do1, l1)
        dh1, ga1 = qkv_back(1, order, dq1, dk1, dv1, cos, sin, h1, dm1, o1, wq, wk, wv)
        dm0, do0, gf0 = ffn_back(0, order, dh1, m0, wo, wg, wu, wd)
        do0, gf1 = lax.optimization_barrier((do0, gf1))
        late = late_weights(me, gf1, weights[4:], m[4:], v[4:])
        all_late = lax.all_gather(late, "dp", axis=0, tiled=False)
        dq0, dk0, dv0 = attend_back(q0, k0, v0, o0, do0, l0)
        _, ga0 = qkv_back(0, order, dq0, dk0, dv0, cos, sin, h0, dm0, o0, wq, wk, wv)
        ga0, _ = lax.optimization_barrier((ga0, late))
        got = sum_blocks(((0, 0), (1, 0), (1, 128), (1, 256), (2, 0)), ga1, gf0, ga0)
        new, new_m, new_v = update(me, got, gf1, weights, m, v)
        out = spread(new, all_late)
        return (*(a.reshape(w.shape) for a, w in zip(out, weights)), *new_m, *new_v)

    states, all_of, cut = P(("rep", "dp"), None, None), P(None, None, None), P(None, "dp", None)
    return jax.shard_map(
        step, mesh=mesh, in_specs=(states, states) + (all_of,) * 7 + (cut,) * 14,
        out_specs=(P("rep", None, None),) * 7 + (P("rep", "dp", None),) * 14, check_vma=False,
    )
```

```python
import functools

import jax
import jax.numpy as jnp
import numpy as np
from jax import lax
from jax.experimental import pallas as pl
from jax.experimental.pallas import tpu as pltpu
from jax.sharding import PartitionSpec as P

LOG2E = 1.4426950408889634
BF, F32 = jnp.bfloat16, jnp.float32
D, HEAD, HEADS, FF, S = 512, 256, 2, 2048, 2048
HALF = HEAD // 2
THETA = 10000
STRIP = 512
N_STRIP = S // STRIP
E = HEAD**-0.5 * LOG2E
HIDDEN = -2e30


def _dot(a, b, ca=1, cb=0):
    return lax.dot_general(a, b, (((ca,), (cb,)), ((), ())), preferred_element_type=F32)


def _scale_of(wide):
    return lax.rsqrt(jnp.mean(wide * wide, -1, keepdims=True) + 1e-6)


def _normed(h):
    wide = h.astype(F32)
    return (wide * _scale_of(wide)).astype(BF)


def _norm_back(h, ct):
    wide = h.astype(F32)
    scale = _scale_of(wide)
    return ct * scale - wide * (scale * scale * scale * jnp.mean(ct * wide, -1, keepdims=True))


def _params(vmem, grid=1):
    return pltpu.CompilerParams(dimension_semantics=("arbitrary",) * grid, vmem_limit_bytes=int(vmem * 2**20))


def _cost(flops, nbytes, trans=0):
    return pl.CostEstimate(flops=int(flops), bytes_accessed=int(nbytes), transcendentals=int(trans))


def _rows(tb, width=D):
    return pl.BlockSpec((tb, width), lambda t: (t, 0))


def _weight(layer, *shape):
    return pl.BlockSpec((None, *shape), lambda *_: (layer, 0, 0))


def _whole(*shape):
    return pl.BlockSpec(shape, lambda *_: (0,) * len(shape))


def _turn(t, cos, sin):
    out = []
    for i in range(HEADS):
        a = t[:, i * HEAD : i * HEAD + HALF].astype(F32)
        b = t[:, i * HEAD + HALF : (i + 1) * HEAD].astype(F32)
        out += [a * cos - b * sin, b * cos + a * sin]
    return jnp.concatenate(out, -1).astype(BF)


def _turn_back(t, cos, sin):
    out = []
    for i in range(HEADS):
        a = t[:, i * HEAD : i * HEAD + HALF].astype(F32)
        b = t[:, i * HEAD + HALF : (i + 1) * HEAD].astype(F32)
        out += [a * cos + b * sin, b * cos - a * sin]
    return jnp.concatenate(out, -1).astype(BF)


def _qkv_kernel(h_ref, cos_ref, sin_ref, wq_ref, wk_ref, wv_ref, q_ref, k_ref, v_ref):
    a = _normed(h_ref[...])
    cos, sin = cos_ref[...], sin_ref[...]
    q_ref[...] = _turn(_dot(a, wq_ref[...]).astype(BF), cos, sin)
    k_ref[...] = _turn(_dot(a, wk_ref[...]).astype(BF), cos, sin)
    v_ref[...] = _dot(a, wv_ref[...]).astype(BF)


def qkv(layer, h, cos, sin, wq, wk, wv, tb=512):
    one = jax.ShapeDtypeStruct((S, D), BF)
    w = _weight(layer, D, D)
    return pl.pallas_call(
        _qkv_kernel, grid=(S // tb,), name="qkv",
        in_specs=[_rows(tb), _rows(tb, HALF), _rows(tb, HALF), w, w, w],
        out_specs=[_rows(tb)] * 3, out_shape=[one] * 3,
        compiler_params=_params(14), cost_estimate=_cost(3 * 2 * S * D * D, 4 * S * D * 2 + 2 * S * HALF * 4),
    )(h, cos, sin, wq, wk, wv)


def _diag():
    shape = (STRIP, STRIP)
    return lax.broadcasted_iota(jnp.int32, shape, 1) >= lax.broadcasted_iota(jnp.int32, shape, 0)


def _attend_kernel(q_ref, k_ref, v_ref, o_ref, lse_ref, vt_s, sc_s, p_s):
    ok = _diag()
    for i in range(HEADS):
        col = slice(i * HEAD, (i + 1) * HEAD)
        vt_s[i, :HEAD, :] = v_ref[:, col].T
        vt_s[i, HEAD:, :] = jnp.ones((16, S), BF)
    for s in range(N_STRIP):
        for i in range(HEADS):
            col = slice(i * HEAD, (i + 1) * HEAD)
            here = slice(s * STRIP, (s + 1) * STRIP)
            n = (s + 1) * STRIP
            q = q_ref[here, col]
            top = None
            for j in range(s + 1):
                sc = _dot(k_ref[j * STRIP : (j + 1) * STRIP, col], q, 1, 1)
                if j == s:
                    sc = jnp.where(ok, sc, HIDDEN)
                sc_s[i, j * STRIP : (j + 1) * STRIP, :] = sc
                m = sc.max(axis=0, keepdims=True)
                top = m if top is None else jnp.maximum(top, m)
            for j in range(s + 1):
                at = slice(j * STRIP, (j + 1) * STRIP)
                p_s[i, at, :] = jnp.exp2((sc_s[i, at, :] - top) * E).astype(BF)
            mix = _dot(vt_s[i, :, :n], p_s[i, :n, :])
            total = mix[HEAD : HEAD + 1, :]
            o_ref[here, col] = (mix[:HEAD, :] * (1 / total)).T.astype(BF)
            lse_ref[i : i + 1, here] = top * (HEAD**-0.5) + jnp.log(total)


def attend(q, k, v):
    return pl.pallas_call(
        _attend_kernel, grid=(1,), name="attend",
        in_specs=[_whole(S, D)] * 3, out_specs=[_whole(S, D), _whole(8, S)],
        out_shape=[jax.ShapeDtypeStruct((S, D), BF), jax.ShapeDtypeStruct((8, S), F32)],
        scratch_shapes=[pltpu.VMEM((HEADS, HEAD + 16, S), BF), pltpu.VMEM((HEADS, S, STRIP), F32), pltpu.VMEM((HEADS, S, STRIP), BF)],
        compiler_params=_params(30), cost_estimate=_cost(2 * HEADS * S * S * HEAD * 1.25, 8 * S * D, HEADS * S * S * 0.6),
    )(q, k, v)


def _attend_back_kernel(q_ref, k_ref, v_ref, o_ref, do_ref, lse_ref, dq_ref, dk_ref, dv_ref, dq_s, p_s, ds_s):
    ok = _diag()
    for i in range(HEADS):
        col = slice(i * HEAD, (i + 1) * HEAD)
        lse = lse_ref[i : i + 1, :] * LOG2E
        deltas = []
        for s in range(N_STRIP):
            here = slice(s * STRIP, (s + 1) * STRIP)
            both = do_ref[here, col].astype(F32) * o_ref[here, col].astype(F32)
            delta = both.sum(-1, keepdims=True)
            deltas.append(jnp.broadcast_to(delta, (STRIP, 128)).T[0:1, :])
        for j in range(N_STRIP):
            at = slice(j * STRIP, (j + 1) * STRIP)
            k, v = k_ref[at, col], v_ref[at, col]
            kt = k.T
            for s in range(j, N_STRIP):
                here = slice(s * STRIP, (s + 1) * STRIP)
                p = jnp.exp2(_dot(k, q_ref[here, col], 1, 1) * E - lse[:, here])
                if s == j:
                    p = jnp.where(ok, p, 0.0)
                dp = _dot(v, do_ref[here, col], 1, 1)
                ds = (p * (dp - deltas[s])).astype(BF)
                p_s[i, :, here] = p.astype(BF)
                ds_s[i, :, here] = ds
                part = _dot(kt, ds)
                if j == 0:
                    dq_s[i, :, here] = part
                else:
                    dq_s[i, :, here] += part
            rest = slice(j * STRIP, S)
            dv_ref[at, col] = _dot(p_s[i, :, rest], do_ref[rest, col]).astype(BF)
            dk_ref[at, col] = (_dot(ds_s[i, :, rest], q_ref[rest, col]) * (HEAD**-0.5)).astype(BF)
        dq_ref[:, col] = (dq_s[i] * (HEAD**-0.5)).T.astype(BF)


def attend_back(q, k, v, o, do, lse):
    one = jax.ShapeDtypeStruct((S, D), BF)
    return pl.pallas_call(
        _attend_back_kernel, grid=(1,), name="attend_back",
        in_specs=[_whole(S, D)] * 5 + [_whole(8, S)], out_specs=[_whole(S, D)] * 3, out_shape=[one] * 3,
        scratch_shapes=[pltpu.VMEM((HEADS, HEAD, S), F32), pltpu.VMEM((HEADS, STRIP, S), BF), pltpu.VMEM((HEADS, STRIP, S), BF)],
        compiler_params=_params(44), cost_estimate=_cost(5 * HEADS * S * S * HEAD * 1.25, 16 * S * D, HEADS * S * S * 0.6),
    )(q, k, v, o, do, lse)


def _project_kernel(h_ref, o_ref, wo_ref, h1_ref):
    h1_ref[...] = (h_ref[...].astype(F32) + _dot(o_ref[...], wo_ref[...]).astype(BF).astype(F32)).astype(BF)


def project(layer, h, o, wo, tb=512):
    return pl.pallas_call(
        _project_kernel, grid=(S // tb,), name="project",
        in_specs=[_rows(tb), _rows(tb), _weight(layer, D, D)], out_specs=_rows(tb), out_shape=jax.ShapeDtypeStruct((S, D), BF),
        compiler_params=_params(8), cost_estimate=_cost(2 * S * D * D, 6 * S * D),
    )(h, o, wo)


def _ffn_kernel(h_ref, o_ref, wo_ref, wg_ref, wu_ref, wd_ref, h1_ref, h2_ref, act_s, *, fc):
    h1 = (h_ref[...].astype(F32) + _dot(o_ref[...], wo_ref[...]).astype(BF).astype(F32)).astype(BF)
    h1_ref[...] = h1
    b = _normed(h1)
    for c in range(FF // fc):
        at = slice(c * fc, (c + 1) * fc)
        gate, up = _dot(b, wg_ref[:, at]), _dot(b, wu_ref[:, at])
        act_s[:, at] = (gate * jax.nn.sigmoid(gate) * up).astype(BF)
    h2_ref[...] = (h1.astype(F32) + _dot(act_s[...], wd_ref[...]).astype(BF).astype(F32)).astype(BF)


def ffn(layer, h, o, wo, wg, wu, wd, tb=512, fc=512):
    one = jax.ShapeDtypeStruct((S, D), BF)
    return pl.pallas_call(
        functools.partial(_ffn_kernel, fc=fc), grid=(S // tb,), name="ffn",
        in_specs=[_rows(tb), _rows(tb), _weight(layer, D, D), _weight(layer, D, FF), _weight(layer, D, FF), _weight(layer, FF, D)],
        out_specs=[_rows(tb)] * 2, out_shape=[one] * 2, scratch_shapes=[pltpu.VMEM((tb, FF), BF)],
        compiler_params=_params(26), cost_estimate=_cost(2 * S * D * (D + 3 * FF), 8 * S * D + 6 * D * FF, S * FF),
    )(h, o, wo, wg, wu, wd)


def _ffn_back_kernel(dy_ref, h1_ref, wo_ref, wg_ref, wu_ref, wd_ref, dh1_ref, do_ref, g_ref, dg_s, du_s, ag_s, au_s, ad_s, *, fc, order):
    t = pl.program_id(0)

    @pl.when(t == 0)
    def _():
        for ref in (ag_s, au_s, ad_s):
            ref[...] = jnp.zeros_like(ref)

    dy, h1 = dy_ref[...], h1_ref[...]
    b = _normed(h1)
    bt, dyt = b.T, dy.T
    for c in range(FF // fc):
        at = slice(c * fc, (c + 1) * fc)
        gate, up = _dot(b, wg_ref[:, at]), _dot(b, wu_ref[:, at])
        dact = _dot(dy, wd_ref[at, :], 1, 1).astype(BF).astype(F32)
        sig = jax.nn.sigmoid(gate)
        silu = gate * sig
        act = (silu * up).astype(BF)
        du = (dact * silu).astype(BF)
        dg = (dact * up * (sig + silu * (1 - sig))).astype(BF)
        dg_s[:, at] = dg
        du_s[:, at] = du
        ag_s[:, at] += _dot(bt, dg)
        au_s[:, at] += _dot(bt, du)
        ad_s[:, at] += _dot(dyt, act)
    db = (_dot(dg_s[...], wg_ref[...], 1, 1) + _dot(du_s[...], wu_ref[...], 1, 1)).astype(BF).astype(F32)
    dh1 = (dy.astype(F32) + _norm_back(h1, db).astype(BF).astype(F32)).astype(BF)
    dh1_ref[...] = dh1
    do_ref[...] = _dot(dh1, wo_ref[...], 1, 1).astype(BF)

    @pl.when(t == pl.num_programs(0) - 1)
    def _():
        n = len(order)
        r, f = D // n, FF // n
        for i, to in enumerate(order):
            for c in range(FF // D):
                at = slice(c * D, (c + 1) * D)
                g_ref[to, c * r : (c + 1) * r, :] = ag_s[i * r : (i + 1) * r, at].astype(BF)
                g_ref[to, f + c * r : f + (c + 1) * r, :] = au_s[i * r : (i + 1) * r, at].astype(BF)
            g_ref[to, 2 * f : 3 * f, :] = ad_s[:, i * f : (i + 1) * f].T.astype(BF)


def ffn_back(layer, order, dy, h1, wo, wg, wu, wd, tb=512, fc=512):
    one, n = jax.ShapeDtypeStruct((S, D), BF), len(order)
    return pl.pallas_call(
        functools.partial(_ffn_back_kernel, fc=fc, order=order), grid=(S // tb,), name="ffn_back",
        in_specs=[_rows(tb), _rows(tb), _weight(layer, D, D), _weight(layer, D, FF), _weight(layer, D, FF), _weight(layer, FF, D)],
        out_specs=[_rows(tb), _rows(tb), _whole(n, 3 * FF // n, D)],
        out_shape=[one, one, jax.ShapeDtypeStruct((n, 3 * FF // n, D), BF)],
        scratch_shapes=[pltpu.VMEM((tb, FF), BF)] * 2 + [pltpu.VMEM((D, FF), F32)] * 3,
        compiler_params=_params(63.9), cost_estimate=_cost(2 * S * D * (D + 8 * FF), 8 * S * D + 12 * D * FF, S * FF),
    )(dy, h1, wo, wg, wu, wd)


def _qkv_back_kernel(dq_ref, dk_ref, dv_ref, cos_ref, sin_ref, h_ref, dh1_ref, o_ref, wq_ref, wk_ref, wv_ref, dh_ref, g_ref, acc_s, *, order):
    t = pl.program_id(0)

    @pl.when(t == 0)
    def _():
        acc_s[...] = jnp.zeros_like(acc_s)

    cos, sin = cos_ref[...], sin_ref[...]
    dq, dk, dv = _turn_back(dq_ref[...], cos, sin), _turn_back(dk_ref[...], cos, sin), dv_ref[...]
    h, dh1 = h_ref[...], dh1_ref[...]
    at = _normed(h).T
    acc_s[0] += _dot(at, dq)
    acc_s[1] += _dot(at, dk)
    acc_s[2] += _dot(at, dv)
    acc_s[3] += _dot(o_ref[...].T, dh1)
    if dh_ref is not None:
        da = (_dot(dq, wq_ref[...], 1, 1) + _dot(dk, wk_ref[...], 1, 1) + _dot(dv, wv_ref[...], 1, 1)).astype(BF).astype(F32)
        dh_ref[...] = (dh1.astype(F32) + _norm_back(h, da).astype(BF).astype(F32)).astype(BF)

    @pl.when(t == pl.num_programs(0) - 1)
    def _():
        r = D // len(order)
        for i, to in enumerate(order):
            for c in range(4):
                g_ref[to, c * r : (c + 1) * r, :] = acc_s[c, i * r : (i + 1) * r, :].astype(BF)


def qkv_back(layer, order, dq, dk, dv, cos, sin, h, dh1, o, wq, wk, wv, tb=512):
    w, first, n = _weight(layer, D, D), layer == 0, len(order)
    packed = jax.ShapeDtypeStruct((n, 4 * D // n, D), BF)
    if first:
        def body(*refs, order):
            _qkv_back_kernel(*refs[:8], None, None, None, None, *refs[8:], order=order)
    else:
        body = _qkv_back_kernel
    given = [dq, dk, dv, cos, sin, h, dh1, o] + ([] if first else [wq, wk, wv])
    got = pl.pallas_call(
        functools.partial(body, order=order), grid=(S // tb,), name="qkv_back",
        in_specs=[_rows(tb)] * 3 + [_rows(tb, HALF)] * 2 + [_rows(tb)] * 3 + ([] if first else [w] * 3),
        out_specs=([] if first else [_rows(tb)]) + [_whole(n, 4 * D // n, D)],
        out_shape=([] if first else [jax.ShapeDtypeStruct((S, D), BF)]) + [packed],
        scratch_shapes=[pltpu.VMEM((4, D, D), F32)],
        compiler_params=_params(24), cost_estimate=_cost(2 * S * D * D * (4 if first else 7), 14 * S * D),
    )(*given)
    return (None, got[0]) if first else got


def tables():
    rate = THETA ** (-np.arange(HALF) / HALF)
    low, high = np.arange(128)[:, None] * rate, np.arange(S // 128)[:, None] * 128 * rate
    cl, sl, ch, sh = (jnp.asarray(f(x), F32) for x in (low, high) for f in (np.cos, np.sin))
    cl, sl, ch, sh = cl[None], sl[None], ch[:, None], sh[:, None]
    return (ch * cl - sh * sl).reshape(S, HALF), (sh * cl + ch * sl).reshape(S, HALF)


CHUNK = 64
NZ = 4


def _place():
    me = lax.axis_index("dp")
    core, chip = lax.rem(me, 2), lax.div(me, 2)
    return core, lax.div(chip, NZ), lax.rem(chip, NZ)


def _peer(core, y, z):
    return lax.axis_index("rep"), (y * NZ + z) * 2 + core


def _greet(core, y, z):
    barrier = pltpu.get_barrier_semaphore()
    peers = [_peer(1 - core, y, z), _peer(core, 1 - y, z)] + [_peer(core, y, lax.rem(z + d, NZ)) for d in range(1, NZ)]
    for peer in peers:
        pl.semaphore_signal(barrier, inc=1, device_id=peer, device_id_type=pl.DeviceIdType.MESH)
    pl.semaphore_wait(barrier, len(peers))


def _send(src, dst, send, recv, peer):
    copy = pltpu.make_async_remote_copy(src_ref=src, dst_ref=dst, send_sem=send, recv_sem=recv, device_id=peer, device_id_type=pl.DeviceIdType.MESH)
    copy.start()
    return copy


def _sum_kernel(*refs, pieces, given):
    g_refs, (out_ref, own, s1, s2, r1, r2, r3, own_sem, d_send, d_recv, y_send, y_recv, z_send, z_recv) = refs[:given], refs[given:]
    core, y, z = _place()
    count = len(pieces)

    def mine(k):
        which, row = pieces[k]
        return g_refs[which], pl.ds(row, CHUNK)

    first, second, third, local = [], [], [], []
    for k in range(count):
        ref, rows = mine(k)
        local.append(pltpu.make_async_copy(ref.at[pl.ds(core * 8, 8), rows], own.at[k], own_sem.at[k]))
        local[k].start()
    _greet(core, y, z)
    for k in range(count):
        ref, rows = mine(k)
        first.append(_send(ref.at[pl.ds((1 - core) * 8, 8), rows], r1.at[k], d_send.at[k], d_recv.at[k], _peer(1 - core, y, z)))
    for k in range(count):
        local[k].wait()
        first[k].wait_recv()

        def add(b, _, k=k):
            s1[k, b] = (own[k, b].astype(F32) + r1[k, b].astype(F32)).astype(BF)
            return _

        lax.fori_loop(0, 8, add, 0)
        second.append(_send(s1.at[k, pl.ds((1 - y) * NZ, NZ)], r2.at[k], y_send.at[k], y_recv.at[k], _peer(core, 1 - y, z)))
    for k in range(count):
        second[k].wait_recv()

        def add(b, _, k=k):
            s2[k, b] = (s1[k, y * NZ + b].astype(F32) + r2[k, b].astype(F32)).astype(BF)
            return _

        lax.fori_loop(0, NZ, add, 0)
        for d in range(1, NZ):
            to = lax.rem(z + d, NZ)
            third.append(_send(s2.at[k, to], r3.at[k, d - 1], z_send.at[k, d - 1], z_recv.at[k, d - 1], _peer(core, y, to)))
    for k in range(count):
        for d in range(NZ - 1):
            third[k * (NZ - 1) + d].wait_recv()
        total = s2[k, z].astype(F32)
        for d in range(NZ - 1):
            total += r3[k, d].astype(F32)
        out_ref[k * CHUNK : (k + 1) * CHUNK, :] = total.astype(BF)
    for copy in first + second + third:
        copy.wait_send()


def sum_blocks(pieces, *packed):
    k = len(pieces)
    vmem = pl.BlockSpec(memory_space=pltpu.VMEM)
    dma = pltpu.SemaphoreType.DMA
    return pl.pallas_call(
        functools.partial(_sum_kernel, pieces=pieces, given=len(packed)), name="sum_blocks",
        in_specs=[pl.BlockSpec(memory_space=pl.ANY)] * len(packed), out_specs=vmem, out_shape=jax.ShapeDtypeStruct((k * CHUNK, D), BF),
        scratch_shapes=[pltpu.VMEM((k, m, CHUNK, D), BF) for m in (8, 8, NZ, 8, NZ, NZ - 1)]
        + [dma((k,)), dma((k,)), dma((k,)), dma((k,)), dma((k,)), dma((k, NZ - 1)), dma((k, NZ - 1))],
        compiler_params=pltpu.CompilerParams(collective_id=1, has_side_effects=True, vmem_limit_bytes=60 * 2**20),
        cost_estimate=_cost(60e9, 2 * 16 * k * CHUNK * D * 2),
    )(*packed)


def _spread_kernel(*refs, layers, pieces):
    (narrow, broad, down, late_ref), out_refs = refs[:4], refs[4 : 4 + pieces]
    own_sem, late_sem, z_send, z_recv, y_send, y_recv, d_send, d_recv = refs[4 + pieces :]
    w_refs = [narrow.at[pl.ds(2 * p, 2)] for p in range(4)] + [broad.at[pl.ds(p, 1)] for p in range(2)] + [down]
    core, y, z = _place()
    at = lambda p, chips: out_refs[p].at[pl.ds(0, layers[p]), chips, core]
    local = [pltpu.make_async_copy(w_refs[p], at(p, y * NZ + z), own_sem.at[p]) for p in range(pieces)]
    r, f = D // 16, FF // 16
    for which in range(2):
        for c in range(FF // D):
            src = late_ref.at[:, :, pl.ds(which * f + c * r, r), :]
            local.append(pltpu.make_async_copy(src, out_refs[4 + which].at[1, :, :, :, pl.ds(c * D, D)], late_sem.at[which * (FF // D) + c]))
    local.append(pltpu.make_async_copy(late_ref.at[:, :, pl.ds(2 * f, f), :], out_refs[6].at[1], late_sem.at[2 * (FF // D)]))
    for copy in local:
        copy.start()
    _greet(core, y, z)
    along, across, over = [], [], []
    for p in range(pieces):
        for d in range(1, NZ):
            along.append(_send(w_refs[p], at(p, y * NZ + z), z_send.at[p, d - 1], z_recv.at[p, d - 1], _peer(core, y, lax.rem(z + d, NZ))))
        across.append([_send(w_refs[p], at(p, y * NZ + z), y_send.at[p, 0], y_recv.at[p, 0], _peer(core, 1 - y, z))])
    for p in range(pieces):
        for d in range(1, NZ):
            along[p * (NZ - 1) + d - 1].wait_recv()
            block = at(p, y * NZ + lax.rem(z + NZ - d, NZ))
            across[p].append(_send(block, block, y_send.at[p, d], y_recv.at[p, d], _peer(core, 1 - y, z)))
        local[p].wait()
        run = at(p, pl.ds(y * NZ, NZ))
        over.append(_send(run, run, d_send.at[p, 0], d_recv.at[p, 0], _peer(1 - core, y, z)))
    for p in range(pieces):
        for copy in across[p]:
            copy.wait_recv()
        run = at(p, pl.ds((1 - y) * NZ, NZ))
        over.append(_send(run, run, d_send.at[p, 1], d_recv.at[p, 1], _peer(1 - core, y, z)))
    for copy in over:
        copy.wait_recv()
    for copy in local[pieces:]:
        copy.wait()
    for copy in along + sum(across, []) + over:
        copy.wait_send()


def spread(given, late):
    shapes = [given[0].shape[1:]] * 4 + [given[1].shape[1:]] * 2 + [given[2].shape[1:]]
    k = len(shapes)
    vmem, hbm = pl.BlockSpec(memory_space=pltpu.VMEM), pl.BlockSpec(memory_space=pl.ANY)
    dma = pltpu.SemaphoreType.DMA
    late = late.reshape(8, 2, *late.shape[1:])
    return pl.pallas_call(
        functools.partial(_spread_kernel, layers=[2] * 4 + [1] * 3, pieces=k), name="spread",
        in_specs=[hbm] * 4, out_specs=[vmem] * k,
        out_shape=[jax.ShapeDtypeStruct((2, 8, 2, *shape), BF) for shape in shapes],
        scratch_shapes=[dma((k,)), dma((2 * FF // D + 1,)), dma((k, NZ - 1)), dma((k, NZ - 1)), dma((k, NZ)), dma((k, NZ)), dma((k, 2)), dma((k, 2))],
        compiler_params=pltpu.CompilerParams(collective_id=2, has_side_effects=True, vmem_limit_bytes=12 * 2**20),
        cost_estimate=_cost(60e9, 16 * 640 * D * 2),
    )(*given, late)


def _store_kernel(*refs, count):
    copies = [pltpu.make_async_copy(refs[i], refs[count + i], refs[-1].at[i]) for i in range(count)]
    for copy in copies:
        copy.start()
    for copy in copies:
        copy.wait()


def store(arrays):
    k = len(arrays)
    return pl.pallas_call(
        functools.partial(_store_kernel, count=k), name="store",
        in_specs=[pl.BlockSpec(memory_space=pltpu.VMEM)] * k, out_specs=[pl.BlockSpec(memory_space=pl.ANY)] * k,
        out_shape=[jax.ShapeDtypeStruct(a.shape, a.dtype) for a in arrays], scratch_shapes=[pltpu.SemaphoreType.DMA((k,))],
        compiler_params=pltpu.CompilerParams(vmem_limit_bytes=20 * 2**20), cost_estimate=_cost(1e9, 34e6),
    )(*arrays)


def adamw(w, m, v, g):
    m = 0.9 * m + 0.1 * g
    v = 0.95 * v + 0.05 * g * g
    step = m * lax.rsqrt(v + 1e-8) + 0.1 * w
    return (w - 0.02 * step).astype(BF), m, v


def _strips(which, n=16):
    r, f = D // n, FF // n
    if which == 2:
        return [(slice(None), slice(0, D), 2 * f)]
    return [(slice(None), slice(c * D, (c + 1) * D), which * f + c * r) for c in range(FF // D)]


def _late_kernel(me_ref, g_ref, *refs):
    w, m, v, (out_ref,) = refs[:3], refs[3:6], refs[6:9], refs[9:]
    for i in range(3):
        for rows, cols, at in _strips(i):
            here = slice(at, at + w[i].shape[0])
            new, _, _ = adamw(w[i][rows, cols].astype(F32), m[i][rows, cols], v[i][rows, cols], g_ref[here, :].astype(F32))
            out_ref[here, :] = new


def late_weights(me, g, w, m, v):
    block = lambda a, own: pl.BlockSpec((None, a.shape[1], a.shape[2]), (lambda i, me: (1, me[0], 0)) if own else (lambda i, me: (1, 0, 0)))
    cut = lambda a, like: pl.BlockSpec((None, like.shape[1], like.shape[2]), lambda i, me: (1, me[0], 0))
    return pl.pallas_call(
        _late_kernel, name="late_weights", out_shape=jax.ShapeDtypeStruct(g.shape, BF),
        grid_spec=pltpu.PrefetchScalarGridSpec(
            num_scalar_prefetch=1, grid=(1,),
            in_specs=[pl.BlockSpec(g.shape, lambda i, me: (0, 0))] + [cut(a, b) for a, b in zip(w, m)] + [block(a, False) for a in (*m, *v)],
            out_specs=pl.BlockSpec(g.shape, lambda i, me: (0, 0))),
        compiler_params=_params(60), cost_estimate=_cost(2e9, 5e6),
    )(me, g, *w, *m, *v)


def _update_kernel(me_ref, got_ref, late_ref, *refs):
    w, m, v = refs[:7], refs[7:14], refs[14:21]
    narrow, broad, down, new_m, new_v = *refs[21:24], refs[24:31], refs[31:38]
    r = D // 16
    for i in range(4):
        for layer, first in ((0, 512), (1, 0)):
            g = got_ref[first + i * r : first + (i + 1) * r, :].astype(F32)
            narrow[2 * i + layer], new_m[i][layer], new_v[i][layer] = adamw(w[i][layer].astype(F32), m[i][layer], v[i][layer], g)
    for i in range(3):
        for rows, cols, at in _strips(i):
            for layer, ref, first in ((0, got_ref, 128), (1, late_ref, 0)):
                here = (layer, rows, cols)
                g = ref[first + at : first + at + m[4 + i].shape[1], :].astype(F32)
                a, b, c = adamw(w[4 + i][here].astype(F32), m[4 + i][here], v[4 + i][here], g)
                new_m[4 + i][here], new_v[4 + i][here] = b, c
                if layer == 0 and i < 2:
                    broad[i, rows, cols] = a
                elif layer == 0:
                    down[0, rows, cols] = a


def update(me, got, late, w, m, v):
    full = lambda a: pl.BlockSpec(a.shape, lambda i, me: (0,) * len(a.shape))
    cut = lambda like: pl.BlockSpec(like.shape, lambda i, me: (0, me[0], 0))
    shape = lambda a, t, count=2: jax.ShapeDtypeStruct((count, *a.shape[1:]), t)
    outs = [shape(m[0], BF, 8), shape(m[4], BF), shape(m[6], BF, 1)] + [shape(a, F32) for a in (*m, *v)]
    out = pl.pallas_call(
        _update_kernel, name="update", out_shape=outs,
        grid_spec=pltpu.PrefetchScalarGridSpec(
            num_scalar_prefetch=1, grid=(1,),
            in_specs=[full(got), full(late)] + [cut(a) for a in m] + [full(a) for a in (*m, *v)],
            out_specs=[full(a) for a in outs]),
        compiler_params=_params(60), cost_estimate=_cost(2e9, 12e6),
    )(me, got, late, *w, *m, *v)
    return out[:3], out[3:10], out[10:]


def solution(mesh):
    n = mesh.shape["dp"]
    plain = tuple(range(n))
    order = tuple((i % 2) * (n // 2) + i // 2 for i in range(n))

    def step(x, dy, wq, wk, wv, wo, wg, wu, wd, *moments):
        weights, m, v = (wq, wk, wv, wo, wg, wu, wd), moments[:7], moments[7:]
        me = lax.axis_index("dp").reshape(1)
        cos, sin = tables()
        h0 = x[0]
        q0, k0, v0 = qkv(0, h0, cos, sin, wq, wk, wv)
        o0, l0 = attend(q0, k0, v0)
        m0, h1 = ffn(0, h0, o0, wo, wg, wu, wd)
        q1, k1, v1 = qkv(1, h1, cos, sin, wq, wk, wv)
        o1, l1 = attend(q1, k1, v1)
        m1 = project(1, h1, o1, wo)
        dm1, do1, gf1 = ffn_back(1, plain, dy[0], m1, wo, wg, wu, wd)
        gf1 = lax.psum_scatter(gf1, "dp", scatter_dimension=0, tiled=False)
        dq1, dk1, dv1 = attend_back(q1, k1, v1, o1, do1, l1)
        dh1, ga1 = qkv_back(1, order, dq1, dk1, dv1, cos, sin, h1, dm1, o1, wq, wk, wv)
        dm0, do0, gf0 = ffn_back(0, order, dh1, m0, wo, wg, wu, wd)
        do0, gf1 = lax.optimization_barrier((do0, gf1))
        late = late_weights(me, gf1, weights[4:], m[4:], v[4:])
        all_late = lax.all_gather(late, "dp", axis=0, tiled=False)
        dq0, dk0, dv0 = attend_back(q0, k0, v0, o0, do0, l0)
        _, ga0 = qkv_back(0, order, dq0, dk0, dv0, cos, sin, h0, dm0, o0, wq, wk, wv)
        ga0, _ = lax.optimization_barrier((ga0, late))
        chunks = [(which, row) for which, g in enumerate((ga1, gf0, ga0)) for row in range(0, g.shape[1], CHUNK)]
        got = sum_blocks(chunks, ga1, gf0, ga0)
        new, new_m, new_v = update(me, got, gf1, weights, m, v)
        out = store(spread(new, all_late))
        return (*(a.reshape(w.shape) for a, w in zip(out, weights)), *new_m, *new_v)

    states, all_of, cut = P(("rep", "dp"), None, None), P(None, None, None), P(None, "dp", None)
    return jax.shard_map(
        step, mesh=mesh, in_specs=(states, states) + (all_of,) * 7 + (cut,) * 14,
        out_specs=(P("rep", None, None),) * 7 + (P("rep", "dp", None),) * 14, check_vma=False,
    )
```
